8 devices in a mesh: dp: 1 (over z), tp: 8 (over y, x, core).
Axes of the slice: x: 2, y: 2, z: 1, core: 2. Of those that a mesh axis runs over, the one named last changes fastest.
Arguments:
- token_ids: int32 [8192], P('dp')
- positions: int32 [8192], P('dp')
- embed_table: bfloat16 [262144, 2560], P('tp')
- norm_scale: float32 [2560], replicated
- w_query: bfloat16 [2560, 2048], P(None, 'tp')
- w_key: bfloat16 [2560, 1024], replicated
- w_value: bfloat16 [2560, 1024], replicated
Outputs:
- output 1: bfloat16 [8192, 2560], P(('dp', 'tp'))
- output 2: bfloat16 [8192, 8, 256], P('dp', 'tp')
- output 3: bfloat16 [8192, 8, 256], P('dp', 'tp')
- output 4: bfloat16 [8192, 8, 256], P('dp', 'tp')
All inputs are finite; a program needn't handle non-finite values.
Results may differ from the reference program's by a relative error of at most 0.0120427.
Values are sent between devices in bfloat16 or wider.
A program may use at most 1 GiB of HBM per device.

```python
import math
import numpy as np
import jax
import jax.numpy as jnp
from jax import lax

D = 2560
HEADS = 8
KV_HEADS = 4
VOCAB = 262144
HEAD_DIM = 256
TOKENS = 8192
KV_SLOTS = 8
START_ODDS = 256
LEVELS = 16

ID_CAPS = np.minimum(VOCAB, 16 * 2 ** np.arange(LEVELS))


def draw_ids(key):
    level_key, id_key = jax.random.split(key)
    levels_drawn = jax.random.randint(level_key, (TOKENS,), 0, LEVELS)
    upper_ids = jnp.asarray(ID_CAPS, dtype=jnp.int32)[levels_drawn]
    token_ids = jax.random.randint(id_key, (TOKENS,), 0, upper_ids, dtype=jnp.int32)
    return token_ids.at[0].set(VOCAB - 1).at[1].set(0)


def draw_positions(key):
    step_ids = jnp.arange(TOKENS, dtype=jnp.int32)
    is_start = jax.random.randint(key, (TOKENS,), 0, START_ODDS, dtype=jnp.int32) == 0
    is_start = is_start.at[0].set(True)
    start_ids = lax.cummax(jnp.where(is_start, step_ids, 0), axis=0)
    return step_ids - start_ids


def setup_inputs(seed: int = 0, part: int = 0) -> dict:
    root_key = jax.random.key(seed)
    part_key = jax.random.fold_in(root_key, part)
    id_key, pos_key = jax.random.split(part_key)
    shared = jax.random.split(root_key, 6)
    row_scale = jax.random.uniform(shared[0], (VOCAB, 1), jnp.float32, 0.25, 2.0)
    embed_table = (jax.random.normal(shared[1], (VOCAB, D), jnp.float32) * (row_scale * D ** -0.5)).astype(jnp.bfloat16)
    norm_scale = 0.5 * jax.random.normal(shared[2], (D,), jnp.float32)
    w_query = (jax.random.normal(shared[3], (D, HEADS * HEAD_DIM), jnp.float32) * D ** -0.5).astype(jnp.bfloat16)
    w_key = (jax.random.normal(shared[4], (D, KV_HEADS * HEAD_DIM), jnp.float32) * D ** -0.5).astype(jnp.bfloat16)
    w_value = (jax.random.normal(shared[5], (D, KV_HEADS * HEAD_DIM), jnp.float32) * D ** -0.5).astype(jnp.bfloat16)
    return {"token_ids": draw_ids(id_key), "positions": draw_positions(pos_key), "embed_table": embed_table, "norm_scale": norm_scale, "w_query": w_query, "w_key": w_key, "w_value": w_value}


def rotate(head_vals, cosines, sines):
    half_dim = HEAD_DIM // 2
    front_half = head_vals[..., :half_dim]
    back_half = head_vals[..., half_dim:]
    return jnp.concatenate([front_half * cosines - back_half * sines, back_half * cosines + front_half * sines], axis=-1)


def reference(token_ids, positions, embed_table, norm_scale, w_query, w_key, w_value):
    normalizer = jnp.asarray(math.sqrt(D), dtype=jnp.bfloat16)
    residual = jnp.take(embed_table, token_ids, axis=0) * normalizer
    widened = residual.astype(jnp.float32)
    inv_rms = lax.rsqrt(jnp.mean(widened * widened, axis=-1, keepdims=True) + 1e-6)
    normed = (widened * inv_rms * (1.0 + norm_scale)).astype(jnp.bfloat16)
    inv_freq = 10000.0 ** (-jnp.arange(0, HEAD_DIM, 2, dtype=jnp.float32) / HEAD_DIM)
    angles = positions.astype(jnp.float32)[:, None] * inv_freq[None, :]
    cosines = jnp.cos(angles)[:, None, :]
    sines = jnp.sin(angles)[:, None, :]
    q_lin = jnp.dot(normed, w_query, preferred_element_type=jnp.float32).astype(jnp.bfloat16)
    k_lin = jnp.dot(normed, w_key, preferred_element_type=jnp.float32).astype(jnp.bfloat16)
    v_lin = jnp.dot(normed, w_value, preferred_element_type=jnp.float32).astype(jnp.bfloat16)
    queries = (rotate(q_lin.reshape(TOKENS, HEADS, HEAD_DIM).astype(jnp.float32), cosines, sines) * HEAD_DIM ** -0.5).astype(jnp.bfloat16)
    keys_rot = rotate(k_lin.reshape(TOKENS, KV_HEADS, HEAD_DIM).astype(jnp.float32), cosines, sines).astype(jnp.bfloat16)
    repeats = KV_SLOTS // KV_HEADS
    key_heads = jnp.repeat(keys_rot, repeats, axis=1)
    value_heads = jnp.repeat(v_lin.reshape(TOKENS, KV_HEADS, HEAD_DIM), repeats, axis=1)
    return (residual, queries, key_heads, value_heads)
```

```python
import functools
import math
import numpy as np
import jax
import jax.numpy as jnp
from jax import lax
from jax.experimental import pallas as pl
from jax.experimental.pallas import tpu as pltpu
from jax.sharding import PartitionSpec as P

HEAD_DIM = 256
EPSILON = 1e-6
ROPE_BASE = 10000.0
MESH = pl.DeviceIdType.MESH

HOT = 1024
CH = 64
CHIP_CHUNKS = (35, 6, 3, 3)
DEV1_CHUNKS = 10
HOT_CHUNKS = HOT // CH
RING_CHUNKS = sum(CHIP_CHUNKS)
RING_ROWS = RING_CHUNKS * CH
ROWS = 2 * RING_ROWS
COLD0_CHUNKS = 2 * CHIP_CHUNKS[0] - DEV1_CHUNKS - HOT_CHUNKS
CAPS = tuple(CH * n for n in (COLD0_CHUNKS, DEV1_CHUNKS, 6, 6, 3, 3, 3, 3))
CAP = max(CAPS)
RING_ORDER = ((0, 1, 3, 2), (0, 2, 3, 1))
BLK = 256
NBLK = -(-RING_ROWS // BLK)
TILE = 128
NTILE = CAP // TILE


def _base_rows():
    base = np.zeros((4, 9), np.int32)
    for chip in range(4):
        for dev in range(9):
            owner, ring = (0, 1) if dev == 8 else (dev // 2, dev % 2)
            order = RING_ORDER[ring]
            pos, src = order.index(chip), order.index(owner)
            hops = (pos - src) % 4
            before = sum(CHIP_CHUNKS[order[(pos - k) % 4]] for k in range(hops))
            base[chip, dev] = ring * RING_ROWS + before * CH
    return base


def _mo(value, step):
    return pl.multiple_of(value, step)


def pack_kernel(flat_ref, par_ref, table, out, pairs, packed, gsem, osem):
    dev = lax.axis_index("tp")
    tiles = jnp.where(dev == 0, NTILE, 0)
    for d in range(1, 8):
        tiles = jnp.where(dev == d, -(-CAPS[d] // TILE), tiles)

    def issue(i):
        def body(j, carry):
            slot = i * TILE + j
            row = flat_ref[slot]
            pltpu.make_async_copy(
                table.at[pl.ds(_mo((row // 2) * 2, 2), 2), :],
                pairs.at[pl.ds(_mo(slot * 2, 2), 2), :], gsem.at[i]).start()
            return carry
        lax.fori_loop(0, TILE, body, 0, unroll=8)

    def out_copy(i):
        here = pl.ds(_mo(i * TILE, TILE), TILE)
        return pltpu.make_async_copy(packed.at[here, :], out.at[here, :], osem.at[i])

    def finish(i):
        both = pl.ds(_mo(i * 2 * TILE, 2 * TILE), 2 * TILE)
        here = pl.ds(_mo(i * TILE, TILE), TILE)
        pltpu.make_async_copy(table.at[pl.ds(0, 2 * TILE), :], pairs.at[both, :], gsem.at[i]).wait()
        row = lax.broadcasted_iota(jnp.int32, (TILE, 2 * TILE), 0)
        col = lax.broadcasted_iota(jnp.int32, (TILE, 2 * TILE), 1)
        pick = jnp.where(col == 2 * row + par_ref[here, :], 1.0, 0.0).astype(jnp.bfloat16)
        packed[here, :] = jnp.dot(pick, pairs[both, :], preferred_element_type=jnp.float32).astype(jnp.bfloat16)
        out_copy(i).start()

    lag = 3

    def step(i, carry):
        @pl.when(i < tiles)
        def _():
            issue(i)

        @pl.when(i >= lag)
        def _():
            finish(i - lag)
        return carry
    lax.fori_loop(0, tiles + lag, step, 0)

    def drain(i, carry):
        out_copy(i).wait()
        return carry
    lax.fori_loop(0, tiles, drain, 0)


def pack_rows(flat, table):
    width = table.shape[1]
    return pl.pallas_call(
        pack_kernel,
        out_shape=jax.ShapeDtypeStruct((CAP, width), jnp.bfloat16),
        in_specs=[pl.BlockSpec(memory_space=pltpu.SMEM), pl.BlockSpec(memory_space=pltpu.VMEM),
                  pl.BlockSpec(memory_space=pl.ANY)],
        out_specs=pl.BlockSpec(memory_space=pl.ANY),
        scratch_shapes=[pltpu.VMEM((2 * CAP, width), jnp.bfloat16), pltpu.VMEM((CAP, width), jnp.bfloat16),
                        pltpu.SemaphoreType.DMA((NTILE,)), pltpu.SemaphoreType.DMA((NTILE,))],
        compiler_params=pltpu.CompilerParams(vmem_limit_bytes=60_000_000),
    )(flat, (flat % 2)[:, None], table)


def ring_kernel(packed, table, idx_ref, scale_ref, wq, wk, wv, lin_out, res_ref,
                rows, acc, wbuf, nbuf, ohbuf, oblk, rsem, nsem, ssem, xsem, osem, wsem):
    width = rows.shape[1]
    tokens = acc.shape[0]
    normalizer = float(np.asarray(math.sqrt(width), dtype=jnp.bfloat16))
    dev = lax.axis_index("tp")
    chip, core = dev // 2, dev % 2
    pos = jnp.where(chip == 0, 0, jnp.where(chip == 3, 2, jnp.where(chip == 1, 1 + 2 * core, 3 - 2 * core)))

    def chip_at(place):
        return jnp.where(place == 0, 0, jnp.where(place == 2, 3, jnp.where(place == 1, 1 + core, 2 - core)))

    def chunks_of(which):
        return jnp.where(which == 0, CHIP_CHUNKS[0], jnp.where(which == 1, CHIP_CHUNKS[1], CHIP_CHUNKS[2]))

    next_chip = chip_at((pos + 1) % 4)
    next_dev = next_chip * 2 + core
    prev_dev = chip_at((pos + 3) % 4) * 2 + core
    sib = chip * 2 + 1 - core
    own = chunks_of(chip)
    n_next = chunks_of(next_chip)
    local = jnp.where(dev == 1, DEV1_CHUNKS, own)
    n_send = RING_CHUNKS - n_next

    barrier = pltpu.get_barrier_semaphore()
    for other in (next_dev, prev_dev, sib):
        pl.semaphore_signal(barrier, inc=1, device_id={"tp": other}, device_id_type=MESH)

    def chunk(ring, i):
        return rows.at[pl.ds(_mo((ring * RING_CHUNKS + i) * CH, CH), CH), :]

    def sem_of(ring, i):
        return rsem.at[ring * RING_CHUNKS + i]

    def wait_chunk(ring, i):
        pltpu.make_async_copy(table.at[pl.ds(0, CH), :], chunk(ring, i), sem_of(ring, i)).wait()

    def to_next(i):
        return pltpu.make_async_remote_copy(
            src_ref=chunk(core, i), dst_ref=chunk(core, i + n_next), send_sem=nsem.at[i],
            recv_sem=sem_of(core, i + n_next), device_id={"tp": next_dev}, device_id_type=MESH)

    def to_sib(i):
        return pltpu.make_async_remote_copy(
            src_ref=chunk(core, i), dst_ref=chunk(core, i), send_sem=ssem.at[i],
            recv_sem=sem_of(core, i), device_id={"tp": sib}, device_id_type=MESH)

    def to_sib_other(i):
        return pltpu.make_async_remote_copy(
            src_ref=chunk(1, i), dst_ref=chunk(1, i), send_sem=xsem.at[i - DEV1_CHUNKS],
            recv_sem=sem_of(1, i), device_id={"tp": sib}, device_id_type=MESH)

    def load(i, carry):
        @pl.when((dev == 0) & (i < HOT_CHUNKS))
        def _():
            pltpu.make_async_copy(table.at[pl.ds(_mo(i * CH, CH), CH), :], chunk(core, i), sem_of(core, i)).start()

        @pl.when((dev != 0) | (i >= HOT_CHUNKS))
        def _():
            first = i - jnp.where(dev == 0, HOT_CHUNKS, 0)
            pltpu.make_async_copy(packed.at[pl.ds(_mo(first * CH, CH), CH), :], chunk(core, i), sem_of(core, i)).start()
        return carry
    lax.fori_loop(0, local, load, 0)

    @pl.when(dev == 0)
    def _():
        def load_other(i, carry):
            first = i - DEV1_CHUNKS + CHIP_CHUNKS[0] - HOT_CHUNKS
            pltpu.make_async_copy(packed.at[pl.ds(_mo(first * CH, CH), CH), :], chunk(1, i), sem_of(1, i)).start()
            return carry
        lax.fori_loop(DEV1_CHUNKS, CHIP_CHUNKS[0], load_other, 0)

    weights = []
    for k, w in enumerate((wq, wk, wv)):
        cols = pl.ds(0, HEAD_DIM) if k == 0 else pl.ds(_mo(chip * HEAD_DIM, HEAD_DIM), HEAD_DIM)
        weights.append(pltpu.make_async_copy(w.at[:, cols], wbuf.at[:, pl.ds(k * HEAD_DIM, HEAD_DIM)], wsem.at[k]))
    for copy in weights:
        copy.start()

    pl.semaphore_wait(barrier, 3)

    def first_sends(i, carry):
        wait_chunk(core, i)
        to_next(i).start()
        return carry
    lax.fori_loop(0, local, first_sends, 0)

    @pl.when(dev == 0)
    def _():
        def send_other(i, carry):
            wait_chunk(1, i)
            to_sib_other(i).start()
            return carry
        lax.fori_loop(DEV1_CHUNKS, CHIP_CHUNKS[0], send_other, 0)

    def first_sib(i, carry):
        to_sib(i).start()
        return carry
    lax.fori_loop(0, local, first_sib, 0)

    acc[...] = jnp.zeros_like(acc)
    for copy in weights:
        copy.wait()

    def relay(i):
        @pl.when((i >= local) & (i < RING_CHUNKS))
        def _():
            wait_chunk(core, i)

            @pl.when(i < n_send)
            def _():
                to_next(i).start()

            @pl.when((dev != 1) | (i >= CHIP_CHUNKS[0]))
            def _():
                to_sib(i).start()

    def lin_copy(first, slot):
        return pltpu.make_async_copy(
            oblk.at[slot], lin_out.at[pl.ds(_mo(first * 8, CH * 8), BLK * 8), :], osem.at[slot])

    def block_start(b):
        return jnp.where(b == NBLK - 1, RING_ROWS - BLK, b * BLK)

    def projections(ring, b, slot, turn):
        first = ring * RING_ROWS + block_start(b)
        gain = 1.0 + scale_ref[...]

        def norm(k, carry):
            emb = rows[pl.ds(_mo(first + k * 32, 32), 32), :].astype(jnp.float32)
            resid = (emb * normalizer).astype(jnp.bfloat16).astype(jnp.float32)
            inv_rms = lax.rsqrt(jnp.mean(resid * resid, axis=-1, keepdims=True) + EPSILON)
            nbuf[pl.ds(_mo(k * 32, 32), 32), :] = (resid * inv_rms * gain).astype(jnp.bfloat16)
            return carry
        lax.fori_loop(0, BLK // 32, norm, 0)

        @pl.when(turn >= 2)
        def _():
            lin_copy(first, slot).wait()
        for k in range(3):
            lin = jnp.dot(nbuf[...], wbuf[:, k * HEAD_DIM:(k + 1) * HEAD_DIM], preferred_element_type=jnp.float32)
            lin = lin.astype(jnp.bfloat16).astype(jnp.float32)
            for half in range(2):
                oblk[slot, pl.ds(2 * k + half, BLK, stride=8), :] = lin[:, half * 128:(half + 1) * 128]
        lin_copy(first, slot).start()

    def pick_tokens(ring, b):
        start = block_start(b)
        first = ring * RING_ROWS + start
        fresh = b * BLK - start
        lane = lax.broadcasted_iota(jnp.int32, (tokens, 128), 1)
        for half in range(2):
            row = lane + half * 128
            hit = (idx_ref[...] - first == row) & (row >= fresh)
            ohbuf[:, half * 128:(half + 1) * 128] = jnp.where(hit, 1.0, 0.0).astype(jnp.bfloat16)

        def part(n, carry):
            cols = pl.ds(_mo(n * 256, 256), 256)
            acc[:, cols] += jnp.dot(ohbuf[...], rows[pl.ds(_mo(first, CH), BLK), cols],
                                    preferred_element_type=jnp.float32)
            return carry
        lax.fori_loop(0, width // 256, part, 0)

    def turn_body(u, carry):
        b, half = u // 2, u % 2
        turn = u - 2
        ring = jnp.where(half == 0, core, 1 - core)
        relay(4 * b + 2 * half)

        @pl.when(turn >= 0)
        def _():
            @pl.when(half == 1)
            def _():
                def wait_one(k, c):
                    i = 4 * (b - 1) + k

                    @pl.when((i < RING_CHUNKS) & ((dev != 0) | (i < DEV1_CHUNKS) | (i >= CHIP_CHUNKS[0])))
                    def _():
                        wait_chunk(1 - core, i)
                    return c
                lax.fori_loop(0, 4, wait_one, 0)
            projections(ring, b - 1, half, turn)
        relay(4 * b + 2 * half + 1)

        @pl.when(turn >= 0)
        def _():
            pick_tokens(ring, b - 1)
        return carry
    lax.fori_loop(0, 2 * NBLK + 2, turn_body, 0)

    def finish(k, carry):
        here = pl.ds(_mo(k * 64, 64), 64)
        res_ref[here, :] = (acc[here, :] * normalizer).astype(jnp.bfloat16)
        return carry
    lax.fori_loop(0, tokens // 64, finish, 0)

    for slot in range(2):
        lin_copy(0, slot).wait()

    def drain_next(i, carry):
        to_next(i).wait_send()
        return carry
    lax.fori_loop(0, n_send, drain_next, 0)

    def drain_sib(i, carry):
        @pl.when((dev != 1) | (i < DEV1_CHUNKS) | (i >= CHIP_CHUNKS[0]))
        def _():
            to_sib(i).wait_send()
        return carry
    lax.fori_loop(0, RING_CHUNKS, drain_sib, 0)

    @pl.when(dev == 0)
    def _():
        def drain_other(i, carry):
            to_sib_other(i).wait_send()
            return carry
        lax.fori_loop(DEV1_CHUNKS, CHIP_CHUNKS[0], drain_other, 0)


def ring_call(packed, table, idx_here, norm_scale, w_query, w_key, w_value):
    width = table.shape[1]
    tokens = idx_here.shape[0]
    anywhere = pl.BlockSpec(memory_space=pl.ANY)
    vmem = pl.BlockSpec(memory_space=pltpu.VMEM)
    return pl.pallas_call(
        ring_kernel,
        out_shape=(jax.ShapeDtypeStruct((ROWS * 8, 128), jnp.float32),
                   jax.ShapeDtypeStruct((tokens, width), jnp.bfloat16)),
        in_specs=[anywhere, anywhere, vmem, vmem, anywhere, anywhere, anywhere],
        out_specs=(anywhere, vmem),
        scratch_shapes=[
            pltpu.VMEM((ROWS, width), jnp.bfloat16),
            pltpu.VMEM((tokens, width), jnp.float32),
            pltpu.VMEM((width, 3 * HEAD_DIM), jnp.bfloat16),
            pltpu.VMEM((BLK, width), jnp.bfloat16),
            pltpu.VMEM((tokens, BLK), jnp.bfloat16),
            pltpu.VMEM((2, BLK * 8, 128), jnp.float32),
            pltpu.SemaphoreType.DMA((2 * RING_CHUNKS,)),
            pltpu.SemaphoreType.DMA((RING_CHUNKS,)),
            pltpu.SemaphoreType.DMA((RING_CHUNKS,)),
            pltpu.SemaphoreType.DMA((CHIP_CHUNKS[0] - DEV1_CHUNKS,)),
            pltpu.SemaphoreType.DMA((2,)),
            pltpu.SemaphoreType.DMA((3,)),
        ],
        compiler_params=pltpu.CompilerParams(collective_id=0, has_side_effects=True, vmem_limit_bytes=67_000_000),
    )(packed, table, jnp.broadcast_to(idx_here[:, None], (tokens, 128)), norm_scale[None, :], w_query, w_key, w_value)


def cos_sin(angle):
    turns = jnp.floor(angle * (2.0 / math.pi) + 0.5)
    rest = ((angle - turns * 1.5703125) - turns * 4.837512969970703125e-4) - turns * 7.54978995489188216e-8
    quarter = turns.astype(jnp.int32)
    z = rest * rest
    s = rest + rest * z * (-1.6666654611e-1 + z * (8.3321608736e-3 + z * -1.9515295891e-4))
    c = 1.0 - 0.5 * z + z * z * (4.166664568298827e-2 + z * (-1.388731625493765e-3 + z * 2.443315711809948e-5))
    odd = (quarter & 1) == 1
    cosine = jnp.where(odd, s, c)
    sine = jnp.where(odd, c, s)
    cosine = jnp.where(((quarter + 1) & 2) == 2, -cosine, cosine)
    sine = jnp.where((quarter & 2) == 2, -sine, sine)
    return cosine, sine


EXPAND = 512
SUB = 64
LOADS = 8


def expand_kernel(idx_ref, pos_ref, freq_ref, lin, q_ref, k_ref, v_ref, table, picked, sem):
    step = pl.program_id(0)
    piece = table.shape[0] // LOADS

    @pl.when(step == 0)
    def _():
        copies = [pltpu.make_async_copy(lin.at[pl.ds(n * piece, piece), :], table.at[pl.ds(n * piece, piece), :],
                                        sem.at[n]) for n in range(LOADS)]
        for copy in copies:
            copy.start()
        for copy in copies:
            copy.wait()

    def take(t, carry):
        row = idx_ref[step * EXPAND + t]
        picked[pl.ds(_mo(t * 8, 8), 8), :] = table[pl.ds(_mo(row * 8, 8), 8), :]
        return carry
    lax.fori_loop(0, EXPAND, take, 0, unroll=16)

    def rope(n, carry):
        here = pl.ds(_mo(n * SUB, SUB), SUB)
        cosines, sines = cos_sin(pos_ref[here, :] * freq_ref[...])
        part = [picked[pl.ds(n * SUB * 8 + s, SUB, stride=8), :] for s in range(6)]
        factor = HEAD_DIM ** -0.5
        q_ref[here, :128] = ((part[0] * cosines - part[1] * sines) * factor).astype(jnp.bfloat16)
        q_ref[here, 128:] = ((part[1] * cosines + part[0] * sines) * factor).astype(jnp.bfloat16)
        k_ref[here, :128] = (part[2] * cosines - part[3] * sines).astype(jnp.bfloat16)
        k_ref[here, 128:] = (part[3] * cosines + part[2] * sines).astype(jnp.bfloat16)
        v_ref[here, :128] = part[4].astype(jnp.bfloat16)
        v_ref[here, 128:] = part[5].astype(jnp.bfloat16)
        return carry
    lax.fori_loop(0, EXPAND // SUB, rope, 0)


def expand(idx, positions, lin):
    tokens = idx.shape[0]
    freq = ROPE_BASE ** (-jnp.arange(0, HEAD_DIM, 2, dtype=jnp.float32) / HEAD_DIM)
    head = jax.ShapeDtypeStruct((tokens, HEAD_DIM), jnp.bfloat16)
    head_spec = pl.BlockSpec((EXPAND, HEAD_DIM), lambda i: (i, 0))
    return pl.pallas_call(
        expand_kernel,
        grid=(tokens // EXPAND,),
        out_shape=(head, head, head),
        in_specs=[pl.BlockSpec(memory_space=pltpu.SMEM), pl.BlockSpec((EXPAND, 1), lambda i: (i, 0)),
                  pl.BlockSpec((1, HEAD_DIM // 2), lambda i: (0, 0)), pl.BlockSpec(memory_space=pl.ANY)],
        out_specs=(head_spec, head_spec, head_spec),
        scratch_shapes=[pltpu.VMEM(lin.shape, jnp.float32), pltpu.VMEM((EXPAND * 8, 128), jnp.float32),
                        pltpu.SemaphoreType.DMA((LOADS,))],
        compiler_params=pltpu.CompilerParams(vmem_limit_bytes=60_000_000),
    )(idx, positions.astype(jnp.float32)[:, None], freq[None, :], lin)


def rope_tables(positions):
    inv_freq = ROPE_BASE ** (-jnp.arange(0, HEAD_DIM, 2, dtype=jnp.float32) / HEAD_DIM)
    angles = positions.astype(jnp.float32)[:, None] * inv_freq[None, :]
    return jnp.cos(angles)[:, None, :], jnp.sin(angles)[:, None, :]


def rotate(head_vals, cosines, sines):
    half_dim = head_vals.shape[-1] // 2
    front_half = head_vals[..., :half_dim]
    back_half = head_vals[..., half_dim:]
    return jnp.concatenate([front_half * cosines - back_half * sines, back_half * cosines + front_half * sines], axis=-1)


def rms_norm(resid_rows, norm_scale):
    widened = resid_rows.astype(jnp.float32)
    inv_rms = lax.rsqrt(jnp.mean(widened * widened, axis=-1, keepdims=True) + EPSILON)
    return (widened * inv_rms * (1.0 + norm_scale)).astype(jnp.bfloat16)


def project(normed, weight, cosines, sines, factor):
    linear = jnp.dot(normed, weight, preferred_element_type=jnp.float32).astype(jnp.bfloat16)
    return (rotate(linear.reshape(linear.shape[0], 1, HEAD_DIM).astype(jnp.float32), cosines, sines) * factor).astype(jnp.bfloat16)


def general(token_ids, positions, table_rows, norm_scale, w_query, w_key, w_value):
    dev = lax.axis_index("tp")
    vocab_rows, width = table_rows.shape
    tokens = token_ids.shape[0]
    normalizer = jnp.asarray(math.sqrt(width), dtype=jnp.bfloat16)
    local_ids = token_ids - dev * vocab_rows
    inside = (local_ids >= 0) & (local_ids < vocab_rows)
    picked = jnp.take(table_rows, local_ids, axis=0, mode="clip") * normalizer
    partial = jnp.where(inside[:, None], picked, jnp.zeros((), jnp.bfloat16))
    parts = lax.all_to_all(partial.reshape(8, tokens // 8, width), "tp", 0, 0)
    residual = jnp.sum(parts.astype(jnp.float32), axis=0).astype(jnp.bfloat16)
    normed = rms_norm(residual, norm_scale)
    normed = lax.all_to_all(jnp.broadcast_to(normed[None], (8,) + normed.shape), "tp", 0, 0).reshape(tokens, width)
    cosines, sines = rope_tables(positions)
    queries = project(normed, w_query, cosines, sines, HEAD_DIM ** -0.5)
    col = (dev // 2) * HEAD_DIM
    key_heads = project(normed, lax.dynamic_slice_in_dim(w_key, col, HEAD_DIM, axis=1), cosines, sines, 1.0)
    value_cols = lax.dynamic_slice_in_dim(w_value, col, HEAD_DIM, axis=1)
    value_heads = jnp.dot(normed, value_cols, preferred_element_type=jnp.float32).astype(jnp.bfloat16)
    return (residual, queries.reshape(tokens, HEAD_DIM), key_heads.reshape(tokens, HEAD_DIM), value_heads)


def solution(mesh):
    base_rows = _base_rows()

    def local_step(token_ids, positions, table_rows, norm_scale, w_query, w_key, w_value):
        dev = lax.axis_index("tp")
        vocab_rows, width = table_rows.shape
        tokens = token_ids.shape[0]
        groups = tokens // 128
        ids = token_ids.reshape(groups, 128)
        owner = ids // vocab_rows
        cold = ids >= HOT
        mine8 = (owner[None] == jnp.arange(8, dtype=jnp.int32)[:, None, None]) & cold[None]
        strict = jnp.asarray(np.triu(np.ones((128, 128)), 1), jnp.bfloat16)
        rank8 = jnp.dot(mine8.astype(jnp.bfloat16).reshape(8 * groups, 128), strict,
                        preferred_element_type=jnp.float32).reshape(8, groups, 128)
        count8 = jnp.sum(mine8.astype(jnp.int32), axis=2)
        offset8 = jnp.sum(jnp.where(np.tri(groups, groups, -1, dtype=bool)[None], count8[:, None, :], 0), axis=2)
        total8 = jnp.sum(count8, axis=1)
        fits = jnp.all(total8 <= jnp.asarray(CAPS, jnp.int32))

        def fast(token_ids, positions, table_rows, norm_scale, w_query, w_key, w_value):
            rank8i = rank8.astype(jnp.int32)
            rank = jnp.sum(jnp.where(mine8, rank8i + offset8[:, :, None], 0), axis=0)
            base = lax.dynamic_index_in_dim(jnp.asarray(base_rows), dev // 2, 0, keepdims=False)
            first = jnp.sum(jnp.where(mine8, base[:8, None, None], 0), axis=0)
            slot0 = jnp.where(cold, HOT + rank, ids)
            split = CHIP_CHUNKS[0] * CH
            idx0 = jnp.where(slot0 < split, base[0] + slot0, base[8] + DEV1_CHUNKS * CH + slot0 - split)
            idx = jnp.where(owner == 0, idx0, first + rank).reshape(tokens)

            mine = lax.dynamic_index_in_dim(mine8, dev, 0, keepdims=False)
            within = lax.dynamic_index_in_dim(rank8i, dev, 0, keepdims=False)
            offset = lax.dynamic_index_in_dim(offset8, dev, 0, keepdims=False)
            count = lax.dynamic_index_in_dim(count8, dev, 0, keepdims=False)
            lane = jnp.arange(128, dtype=jnp.int32)
            place = jnp.where(mine, within, -1)
            local = ids - dev * vocab_rows
            listed = jnp.sum(jnp.where(place[:, None, :] == lane[None, :, None], local[:, None, :], 0), axis=2)
            slot = jnp.arange(CAP, dtype=jnp.int32)[:, None]
            group = (offset[None] <= slot) & (slot < (offset + count)[None])
            digits = jnp.concatenate([listed // 256, listed % 256], axis=1).astype(jnp.bfloat16)
            found = jnp.dot(group.astype(jnp.bfloat16), digits, preferred_element_type=jnp.float32)
            found = (found[:, :128] * 256.0 + found[:, 128:]).astype(jnp.int32)
            column = slot - jnp.sum(jnp.where(group, offset[None], 0), axis=1, keepdims=True)
            flat = jnp.sum(jnp.where(column == lane[None], found, 0), axis=1)

            packed = pack_rows(flat, table_rows)
            share = tokens // 8
            idx_here = lax.dynamic_slice_in_dim(idx, dev * share, share)
            lin, residual = ring_call(packed, table_rows, idx_here, norm_scale, w_query, w_key, w_value)
            queries, key_heads, value_heads = expand(idx, positions, lin)
            return residual, queries, key_heads, value_heads

        outs = lax.cond(fits, fast, general, token_ids, positions, table_rows, norm_scale, w_query, w_key, w_value)
        residual, heads = outs[0], outs[1:]
        return (residual,) + tuple(h.reshape(tokens, 1, HEAD_DIM) for h in heads)

    head_spec = P("dp", "tp", None)
    return jax.shard_map(local_step, mesh=mesh, in_specs=(P("dp"), P("dp"), P("tp", None), P(), P(None, "tp"), P(), P()), out_specs=(P(("dp", "tp"), None), head_spec, head_spec, head_spec), check_vma=False)
```

```python
import functools
import math
import numpy as np
import jax
import jax.numpy as jnp
from jax import lax
from jax.experimental import pallas as pl
from jax.experimental.pallas import tpu as pltpu
from jax.sharding import PartitionSpec as P

HEAD_DIM = 256
EPSILON = 1e-6
ROPE_BASE = 10000.0
MESH = pl.DeviceIdType.MESH

HOT = 1024
CH = 64
CHIP_CHUNKS = (35, 6, 3, 3)
DEV1_CHUNKS = 10
HOT_CHUNKS = HOT // CH
RING_CHUNKS = sum(CHIP_CHUNKS)
RING_ROWS = RING_CHUNKS * CH
ROWS = 2 * RING_ROWS
COLD0_CHUNKS = 2 * CHIP_CHUNKS[0] - DEV1_CHUNKS - HOT_CHUNKS
CAPS = tuple(CH * n for n in (COLD0_CHUNKS, DEV1_CHUNKS, 6, 6, 3, 3, 3, 3))
CAP = max(CAPS)
RING_ORDER = ((0, 1, 3, 2), (0, 2, 3, 1))
BLK = 128
NBLK = -(-RING_ROWS // BLK)
TILE = 128
NTILE = CAP // TILE


def _base_rows():
    base = np.zeros((4, 9), np.int32)
    for chip in range(4):
        for dev in range(9):
            owner, ring = (0, 1) if dev == 8 else (dev // 2, dev % 2)
            order = RING_ORDER[ring]
            pos, src = order.index(chip), order.index(owner)
            hops = (pos - src) % 4
            before = sum(CHIP_CHUNKS[order[(pos - k) % 4]] for k in range(hops))
            base[chip, dev] = ring * RING_ROWS + before * CH
    return base


def _mo(value, step):
    return pl.multiple_of(value, step)


def start_pairs(count, row_of, source, pairs, first, sem):
    def body(j, carry):
        into = pairs.at[pl.ds(_mo(first + 16 * j, 16), 16), :]
        for k in range(8):
            even = row_of(8 * j + k) & -2
            pltpu.make_async_copy(
                source.at[pl.ds(_mo(even, 2), 2), :], into.at[pl.ds(2 * k, 2), :], sem).start(priority=k % 2)
        return carry
    lax.fori_loop(0, count // 8, body, 0)


def pick_odd(rows_row, count):
    odd = jnp.transpose(jnp.broadcast_to(rows_row & 1, (128, 128)))[:count, :]
    row = lax.broadcasted_iota(jnp.int32, (count, 128), 0)
    col = lax.broadcasted_iota(jnp.int32, (count, 128), 1)
    halves = [jnp.where(col + part == 2 * row + odd, 1.0, 0.0) for part in range(0, 2 * count, 128)]
    return jnp.concatenate(halves, axis=1).astype(jnp.bfloat16)


def pack_kernel(flat_ref, rows_ref, table, out, pairs, packed, gsem, osem):
    dev = lax.axis_index("tp")
    tiles = jnp.where(dev == 0, NTILE, 0)
    for d in range(1, 8):
        tiles = jnp.where(dev == d, -(-CAPS[d] // TILE), tiles)

    def issue(i):
        start_pairs(TILE, lambda j: flat_ref[i * TILE + j], table, pairs, i * 2 * TILE, gsem.at[i])

    def out_copy(i):
        here = pl.ds(_mo(i * TILE, TILE), TILE)
        return pltpu.make_async_copy(packed.at[here, :], out.at[here, :], osem.at[i])

    def finish(i):
        both = pl.ds(_mo(i * 2 * TILE, 2 * TILE), 2 * TILE)
        here = pl.ds(_mo(i * TILE, TILE), TILE)
        pltpu.make_async_copy(table.at[pl.ds(0, 2 * TILE), :], pairs.at[both, :], gsem.at[i]).wait()
        pick = pick_odd(rows_ref[pl.ds(i, 1), :], TILE)
        packed[here, :] = jnp.dot(pick, pairs[both, :], preferred_element_type=jnp.float32).astype(jnp.bfloat16)
        out_copy(i).start()

    lag = 3

    def step(i, carry):
        @pl.when(i < tiles)
        def _():
            issue(i)

        @pl.when(i >= lag)
        def _():
            finish(i - lag)
        return carry
    lax.fori_loop(0, tiles + lag, step, 0)

    def drain(i, carry):
        out_copy(i).wait()
        return carry
    lax.fori_loop(0, tiles, drain, 0)


def pack_rows(flat, table):
    width = table.shape[1]
    return pl.pallas_call(
        pack_kernel,
        out_shape=jax.ShapeDtypeStruct((CAP, width), jnp.bfloat16),
        in_specs=[pl.BlockSpec(memory_space=pltpu.SMEM), pl.BlockSpec(memory_space=pltpu.VMEM),
                  pl.BlockSpec(memory_space=pl.ANY)],
        out_specs=pl.BlockSpec(memory_space=pl.ANY),
        scratch_shapes=[pltpu.VMEM((2 * CAP, width), jnp.bfloat16), pltpu.VMEM((CAP, width), jnp.bfloat16),
                        pltpu.SemaphoreType.DMA((NTILE,)), pltpu.SemaphoreType.DMA((NTILE,))],
        compiler_params=pltpu.CompilerParams(vmem_limit_bytes=60_000_000),
    )(flat, flat.reshape(NTILE, TILE), table)


def ring_kernel(packed, table, pos_ref, freq_ref, scale_ref, wq, wk, wv, lin_out, rows_out, rope_out,
                rows, wbuf, nbuf, oblk, rope_buf, rsem, nsem, ssem, xsem, osem, ksem, psem, wsem):
    width = rows.shape[1]
    normalizer = float(np.asarray(math.sqrt(width), dtype=jnp.bfloat16))
    dev = lax.axis_index("tp")
    chip, core = dev // 2, dev % 2
    pos = jnp.where(chip == 0, 0, jnp.where(chip == 3, 2, jnp.where(chip == 1, 1 + 2 * core, 3 - 2 * core)))

    def chip_at(place):
        return jnp.where(place == 0, 0, jnp.where(place == 2, 3, jnp.where(place == 1, 1 + core, 2 - core)))

    def chunks_of(which):
        return jnp.where(which == 0, CHIP_CHUNKS[0], jnp.where(which == 1, CHIP_CHUNKS[1], CHIP_CHUNKS[2]))

    next_chip = chip_at((pos + 1) % 4)
    next_dev = next_chip * 2 + core
    prev_dev = chip_at((pos + 3) % 4) * 2 + core
    sib = chip * 2 + 1 - core
    own = chunks_of(chip)
    n_next = chunks_of(next_chip)
    local = jnp.where(dev == 1, DEV1_CHUNKS, own)
    n_send = RING_CHUNKS - n_next

    barrier = pltpu.get_barrier_semaphore()
    for other in (next_dev, prev_dev, sib):
        pl.semaphore_signal(barrier, inc=1, device_id={"tp": other}, device_id_type=MESH)

    def chunk(ring, i):
        return rows.at[pl.ds(_mo((ring * RING_CHUNKS + i) * CH, CH), CH), :]

    def sem_of(ring, i):
        return rsem.at[ring * RING_CHUNKS + i]

    def wait_chunk(ring, i):
        pltpu.make_async_copy(table.at[pl.ds(0, CH), :], chunk(ring, i), sem_of(ring, i)).wait()

    def to_next(i):
        return pltpu.make_async_remote_copy(
            src_ref=chunk(core, i), dst_ref=chunk(core, i + n_next), send_sem=nsem.at[i],
            recv_sem=sem_of(core, i + n_next), device_id={"tp": next_dev}, device_id_type=MESH)

    def to_sib(i):
        return pltpu.make_async_remote_copy(
            src_ref=chunk(core, i), dst_ref=chunk(core, i), send_sem=ssem.at[i],
            recv_sem=sem_of(core, i), device_id={"tp": sib}, device_id_type=MESH)

    def to_sib_other(i):
        return pltpu.make_async_remote_copy(
            src_ref=chunk(1, i), dst_ref=chunk(1, i), send_sem=xsem.at[i - DEV1_CHUNKS],
            recv_sem=sem_of(1, i), device_id={"tp": sib}, device_id_type=MESH)

    def load(i, carry):
        @pl.when((dev == 0) & (i < HOT_CHUNKS))
        def _():
            pltpu.make_async_copy(table.at[pl.ds(_mo(i * CH, CH), CH), :], chunk(core, i), sem_of(core, i)).start()

        @pl.when((dev != 0) | (i >= HOT_CHUNKS))
        def _():
            first = i - jnp.where(dev == 0, HOT_CHUNKS, 0)
            pltpu.make_async_copy(packed.at[pl.ds(_mo(first * CH, CH), CH), :], chunk(core, i), sem_of(core, i)).start()
        return carry
    lax.fori_loop(0, local, load, 0)

    @pl.when(dev == 0)
    def _():
        def load_other(i, carry):
            first = i - DEV1_CHUNKS + CHIP_CHUNKS[0] - HOT_CHUNKS
            pltpu.make_async_copy(packed.at[pl.ds(_mo(first * CH, CH), CH), :], chunk(1, i), sem_of(1, i)).start()
            return carry
        lax.fori_loop(DEV1_CHUNKS, CHIP_CHUNKS[0], load_other, 0)

    weights = []
    for k, w in enumerate((wq, wk, wv)):
        cols = pl.ds(0, HEAD_DIM) if k == 0 else pl.ds(_mo(chip * HEAD_DIM, HEAD_DIM), HEAD_DIM)
        weights.append(pltpu.make_async_copy(w.at[:, cols], wbuf.at[:, pl.ds(k * HEAD_DIM, HEAD_DIM)], wsem.at[k]))
    for copy in weights:
        copy.start()

    pl.semaphore_wait(barrier, 3)

    def first_sends(i, carry):
        wait_chunk(core, i)
        to_next(i).start()
        return carry
    lax.fori_loop(0, local, first_sends, 0)

    @pl.when(dev == 0)
    def _():
        def send_other(i, carry):
            wait_chunk(1, i)
            to_sib_other(i).start()
            return carry
        lax.fori_loop(DEV1_CHUNKS, CHIP_CHUNKS[0], send_other, 0)

    def first_sib(i, carry):
        to_sib(i).start()
        return carry
    lax.fori_loop(0, local, first_sib, 0)

    for copy in weights:
        copy.wait()

    def relay(i):
        @pl.when((i >= local) & (i < RING_CHUNKS))
        def _():
            wait_chunk(core, i)

            @pl.when(i < n_send)
            def _():
                to_next(i).start()

            @pl.when((dev != 1) | (i >= CHIP_CHUNKS[0]))
            def _():
                to_sib(i).start()

    def lin_copy(first, slot):
        return pltpu.make_async_copy(
            oblk.at[slot], lin_out.at[pl.ds(_mo(first * 8, CH * 8), BLK * 8), :], osem.at[slot])

    def keep_copy(first, slot):
        here = pl.ds(_mo(first, CH), BLK)
        return pltpu.make_async_copy(rows.at[here, :], rows_out.at[here, :], ksem.at[slot])

    def rope_copy(group, slot):
        return pltpu.make_async_copy(
            rope_buf.at[slot], rope_out.at[pl.ds(_mo(group * 128, 128), 128), :], psem.at[slot])

    def rope_tables_of(group, slot):
        angle = jnp.transpose(jnp.broadcast_to(pos_ref[pl.ds(group, 1), :], (128, 128))) * freq_ref[...]
        cosine, sine = cos_sin(angle)

        @pl.when(group >= 2)
        def _():
            rope_copy(group, slot).wait()
        rope_buf[slot, :, :128] = cosine
        rope_buf[slot, :, 128:] = sine
        rope_copy(group, slot).start()

    def block_start(b):
        return jnp.where(b == NBLK - 1, RING_ROWS - BLK, b * BLK)

    def projections(ring, b, slot, turn):
        first = ring * RING_ROWS + block_start(b)
        gain = 1.0 + scale_ref[...]

        def norm(k, carry):
            emb = rows[pl.ds(_mo(first + k * 32, 32), 32), :].astype(jnp.float32)
            resid = (emb * normalizer).astype(jnp.bfloat16).astype(jnp.float32)
            inv_rms = lax.rsqrt(jnp.mean(resid * resid, axis=-1, keepdims=True) + EPSILON)
            nbuf[pl.ds(_mo(k * 32, 32), 32), :] = (resid * inv_rms * gain).astype(jnp.bfloat16)
            return carry
        lax.fori_loop(0, BLK // 32, norm, 0)

        @pl.when(turn >= 2)
        def _():
            lin_copy(first, slot).wait()
            keep_copy(first, slot).wait()
        keep_copy(first, slot).start()
        for k in range(3):
            lin = jnp.dot(nbuf[...], wbuf[:, k * HEAD_DIM:(k + 1) * HEAD_DIM], preferred_element_type=jnp.float32)
            lin = lin.astype(jnp.bfloat16).astype(jnp.float32)
            for half in range(2):
                oblk[slot, pl.ds(2 * k + half, BLK, stride=8), :] = lin[:, half * 128:(half + 1) * 128]
        lin_copy(first, slot).start()

    def turn_body(u, carry):
        b, half = u // 2, u % 2
        turn = u - 2
        ring = jnp.where(half == 0, core, 1 - core)
        relay(u)

        @pl.when(turn >= 0)
        def _():
            @pl.when(half == 1)
            def _():
                def wait_one(k, c):
                    i = 2 * (b - 1) + k

                    @pl.when((i < RING_CHUNKS) & ((dev != 0) | (i < DEV1_CHUNKS) | (i >= CHIP_CHUNKS[0])))
                    def _():
                        wait_chunk(1 - core, i)
                    return c
                lax.fori_loop(0, 2, wait_one, 0)
            projections(ring, b - 1, half, turn)

        @pl.when((b >= 2) & (b < 2 + pos_ref.shape[0] // 4))
        def _():
            for k in range(2):
                rope_tables_of((u - 4) * 2 + k, k)
        return carry
    lax.fori_loop(0, 2 * NBLK + 2, turn_body, 0)

    for slot in range(2):
        lin_copy(0, slot).wait()
        keep_copy(0, slot).wait()
        rope_copy(0, slot).wait()

    def drain_next(i, carry):
        to_next(i).wait_send()
        return carry
    lax.fori_loop(0, n_send, drain_next, 0)

    def drain_sib(i, carry):
        @pl.when((dev != 1) | (i < DEV1_CHUNKS) | (i >= CHIP_CHUNKS[0]))
        def _():
            to_sib(i).wait_send()
        return carry
    lax.fori_loop(0, RING_CHUNKS, drain_sib, 0)

    @pl.when(dev == 0)
    def _():
        def drain_other(i, carry):
            to_sib_other(i).wait_send()
            return carry
        lax.fori_loop(DEV1_CHUNKS, CHIP_CHUNKS[0], drain_other, 0)


def ring_call(packed, table, positions, norm_scale, w_query, w_key, w_value):
    width = table.shape[1]
    tokens = positions.shape[0]
    freq = ROPE_BASE ** (-jnp.arange(0, HEAD_DIM, 2, dtype=jnp.float32) / HEAD_DIM)
    anywhere = pl.BlockSpec(memory_space=pl.ANY)
    vmem = pl.BlockSpec(memory_space=pltpu.VMEM)
    return pl.pallas_call(
        ring_kernel,
        out_shape=(jax.ShapeDtypeStruct((ROWS * 8, 128), jnp.float32),
                   jax.ShapeDtypeStruct((ROWS, width), jnp.bfloat16),
                   jax.ShapeDtypeStruct((tokens, HEAD_DIM), jnp.float32)),
        in_specs=[anywhere, anywhere, vmem, vmem, vmem, anywhere, anywhere, anywhere],
        out_specs=(anywhere, anywhere, anywhere),
        scratch_shapes=[
            pltpu.VMEM((ROWS, width), jnp.bfloat16),
            pltpu.VMEM((width, 3 * HEAD_DIM), jnp.bfloat16),
            pltpu.VMEM((BLK, width), jnp.bfloat16),
            pltpu.VMEM((2, BLK * 8, 128), jnp.float32),
            pltpu.VMEM((2, 128, HEAD_DIM), jnp.float32),
            pltpu.SemaphoreType.DMA((2 * RING_CHUNKS,)),
            pltpu.SemaphoreType.DMA((RING_CHUNKS,)),
            pltpu.SemaphoreType.DMA((RING_CHUNKS,)),
            pltpu.SemaphoreType.DMA((CHIP_CHUNKS[0] - DEV1_CHUNKS,)),
            pltpu.SemaphoreType.DMA((2,)),
            pltpu.SemaphoreType.DMA((2,)),
            pltpu.SemaphoreType.DMA((2,)),
            pltpu.SemaphoreType.DMA((3,)),
        ],
        compiler_params=pltpu.CompilerParams(collective_id=0, has_side_effects=True, vmem_limit_bytes=60_000_000),
    )(packed, table, positions.astype(jnp.float32).reshape(tokens // 128, 128), freq[None, :], norm_scale[None, :],
      w_query, w_key, w_value)


def cos_sin(angle):
    turns = jnp.floor(angle * (2.0 / math.pi) + 0.5)
    rest = ((angle - turns * 1.5703125) - turns * 4.837512969970703125e-4) - turns * 7.54978995489188216e-8
    quarter = turns.astype(jnp.int32)
    z = rest * rest
    s = rest + rest * z * (-1.6666654611e-1 + z * (8.3321608736e-3 + z * -1.9515295891e-4))
    c = 1.0 - 0.5 * z + z * z * (4.166664568298827e-2 + z * (-1.388731625493765e-3 + z * 2.443315711809948e-5))
    odd = (quarter & 1) == 1
    cosine = jnp.where(odd, s, c)
    sine = jnp.where(odd, c, s)
    cosine = jnp.where(((quarter + 1) & 2) == 2, -cosine, cosine)
    sine = jnp.where((quarter & 2) == 2, -sine, sine)
    return cosine, sine


EXPAND = 512
SUB = 64
SHARE = 64
LOADS = 8


def expand_kernel(idx_ref, here_ref, rope_ref, lin, rows, res_ref, q_ref, k_ref, v_ref,
                  table, even, odd, pairs, sem, gsem):
    step, steps = pl.program_id(0), pl.num_programs(0)
    first = lax.axis_index("tp") * (steps * SHARE)
    piece = table.shape[0] // LOADS
    tiles = EXPAND // SUB
    last = steps * tiles - 1

    def start_share(n):
        start_pairs(SHARE, lambda j: idx_ref[first + n * SHARE + j], rows, pairs, n * 2 * SHARE, gsem.at[n])

    def take(tile, picked):
        for t in range(SUB):
            row = idx_ref[tile * SUB + t]
            picked[8 * t:8 * t + 8, :] = table[pl.ds(_mo(row * 8, 8), 8), :]

    @pl.when(step == 0)
    def _():
        copies = [pltpu.make_async_copy(lin.at[pl.ds(n * piece, piece), :], table.at[pl.ds(n * piece, piece), :],
                                        sem.at[n]) for n in range(LOADS)]
        for n, copy in enumerate(copies):
            copy.start(priority=n % 2)
        def start_one(n, carry):
            start_share(n)
            return carry
        lax.fori_loop(0, steps, start_one, 0)
        for copy in copies:
            copy.wait()
        take(0, even)

    def rope(n, picked):
        here = pl.ds(_mo(n * SUB, SUB), SUB)
        cosines, sines = rope_ref[here, :128], rope_ref[here, 128:]
        part = [picked[pl.ds(s, SUB, stride=8), :] for s in range(6)]
        factor = HEAD_DIM ** -0.5
        q_ref[here, :128] = ((part[0] * cosines - part[1] * sines) * factor).astype(jnp.bfloat16)
        q_ref[here, 128:] = ((part[1] * cosines + part[0] * sines) * factor).astype(jnp.bfloat16)
        k_ref[here, :128] = (part[2] * cosines - part[3] * sines).astype(jnp.bfloat16)
        k_ref[here, 128:] = (part[3] * cosines + part[2] * sines).astype(jnp.bfloat16)
        v_ref[here, :128] = part[4].astype(jnp.bfloat16)
        v_ref[here, 128:] = part[5].astype(jnp.bfloat16)

    def two_tiles(n, carry):
        tile = step * tiles + 2 * n
        take(tile + 1, odd)
        rope(2 * n, even)
        take(jnp.minimum(tile + 2, last), even)
        rope(2 * n + 1, odd)
        return carry
    lax.fori_loop(0, tiles // 2, two_tiles, 0)

    share = pairs.at[pl.ds(_mo(step * 2 * SHARE, 2 * SHARE), 2 * SHARE), :]
    pltpu.make_async_copy(rows.at[pl.ds(0, 2 * SHARE), :], share, gsem.at[step]).wait()
    normalizer = float(np.asarray(math.sqrt(rows.shape[1]), dtype=jnp.bfloat16))
    half = jnp.where(step % 2 == 0, here_ref[pl.ds(step // 2, 1), :], pltpu.roll(here_ref[pl.ds(step // 2, 1), :], 128 - SHARE, 1))
    emb = jnp.dot(pick_odd(half, SHARE), share[...], preferred_element_type=jnp.float32)
    res_ref[...] = (emb * normalizer).astype(jnp.bfloat16)


def expand(idx, idx_here, rope, lin, rows):
    tokens, width = idx.shape[0], rows.shape[1]
    steps = tokens // EXPAND
    head = jax.ShapeDtypeStruct((tokens, HEAD_DIM), jnp.bfloat16)
    head_spec = pl.BlockSpec((EXPAND, HEAD_DIM), lambda i: (i, 0))
    return pl.pallas_call(
        expand_kernel,
        grid=(steps,),
        out_shape=(jax.ShapeDtypeStruct((steps * SHARE, width), jnp.bfloat16), head, head, head),
        in_specs=[pl.BlockSpec(memory_space=pltpu.SMEM), pl.BlockSpec(memory_space=pltpu.VMEM),
                  pl.BlockSpec((EXPAND, HEAD_DIM), lambda i: (i, 0)),
                  pl.BlockSpec(memory_space=pl.ANY), pl.BlockSpec(memory_space=pl.ANY)],
        out_specs=(pl.BlockSpec((SHARE, width), lambda i: (i, 0)), head_spec, head_spec, head_spec),
        scratch_shapes=[pltpu.VMEM(lin.shape, jnp.float32), pltpu.VMEM((SUB * 8, 128), jnp.float32),
                        pltpu.VMEM((SUB * 8, 128), jnp.float32), pltpu.VMEM((steps * 2 * SHARE, width), jnp.bfloat16),
                        pltpu.SemaphoreType.DMA((LOADS,)), pltpu.SemaphoreType.DMA((steps,))],
        compiler_params=pltpu.CompilerParams(vmem_limit_bytes=60_000_000),
    )(idx, idx_here.reshape(-1, 128), rope, lin, rows)


def rope_tables(positions):
    inv_freq = ROPE_BASE ** (-jnp.arange(0, HEAD_DIM, 2, dtype=jnp.float32) / HEAD_DIM)
    angles = positions.astype(jnp.float32)[:, None] * inv_freq[None, :]
    return jnp.cos(angles)[:, None, :], jnp.sin(angles)[:, None, :]


def rotate(head_vals, cosines, sines):
    half_dim = head_vals.shape[-1] // 2
    front_half = head_vals[..., :half_dim]
    back_half = head_vals[..., half_dim:]
    return jnp.concatenate([front_half * cosines - back_half * sines, back_half * cosines + front_half * sines], axis=-1)


def rms_norm(resid_rows, norm_scale):
    widened = resid_rows.astype(jnp.float32)
    inv_rms = lax.rsqrt(jnp.mean(widened * widened, axis=-1, keepdims=True) + EPSILON)
    return (widened * inv_rms * (1.0 + norm_scale)).astype(jnp.bfloat16)


def project(normed, weight, cosines, sines, factor):
    linear = jnp.dot(normed, weight, preferred_element_type=jnp.float32).astype(jnp.bfloat16)
    return (rotate(linear.reshape(linear.shape[0], 1, HEAD_DIM).astype(jnp.float32), cosines, sines) * factor).astype(jnp.bfloat16)


def general(token_ids, positions, table_rows, norm_scale, w_query, w_key, w_value):
    dev = lax.axis_index("tp")
    vocab_rows, width = table_rows.shape
    tokens = token_ids.shape[0]
    normalizer = jnp.asarray(math.sqrt(width), dtype=jnp.bfloat16)
    local_ids = token_ids - dev * vocab_rows
    inside = (local_ids >= 0) & (local_ids < vocab_rows)
    picked = jnp.take(table_rows, local_ids, axis=0, mode="clip") * normalizer
    partial = jnp.where(inside[:, None], picked, jnp.zeros((), jnp.bfloat16))
    parts = lax.all_to_all(partial.reshape(8, tokens // 8, width), "tp", 0, 0)
    residual = jnp.sum(parts.astype(jnp.float32), axis=0).astype(jnp.bfloat16)
    normed = rms_norm(residual, norm_scale)
    normed = lax.all_to_all(jnp.broadcast_to(normed[None], (8,) + normed.shape), "tp", 0, 0).reshape(tokens, width)
    cosines, sines = rope_tables(positions)
    queries = project(normed, w_query, cosines, sines, HEAD_DIM ** -0.5)
    col = (dev // 2) * HEAD_DIM
    key_heads = project(normed, lax.dynamic_slice_in_dim(w_key, col, HEAD_DIM, axis=1), cosines, sines, 1.0)
    value_cols = lax.dynamic_slice_in_dim(w_value, col, HEAD_DIM, axis=1)
    value_heads = jnp.dot(normed, value_cols, preferred_element_type=jnp.float32).astype(jnp.bfloat16)
    return (residual, queries.reshape(tokens, HEAD_DIM), key_heads.reshape(tokens, HEAD_DIM), value_heads)


def solution(mesh):
    base_rows = _base_rows()

    def local_step(token_ids, positions, table_rows, norm_scale, w_query, w_key, w_value):
        dev = lax.axis_index("tp")
        vocab_rows, width = table_rows.shape
        tokens = token_ids.shape[0]
        groups = tokens // 128
        ids = token_ids.reshape(groups, 128)
        owner = ids // vocab_rows
        cold = ids >= HOT
        mine8 = (owner[None] == jnp.arange(8, dtype=jnp.int32)[:, None, None]) & cold[None]
        strict = jnp.asarray(np.triu(np.ones((128, 128)), 1), jnp.bfloat16)
        rank8 = jnp.dot(mine8.astype(jnp.bfloat16).reshape(8 * groups, 128), strict,
                        preferred_element_type=jnp.float32).reshape(8, groups, 128)
        count8 = jnp.sum(mine8.astype(jnp.int32), axis=2)
        offset8 = jnp.sum(jnp.where(np.tri(groups, groups, -1, dtype=bool)[None], count8[:, None, :], 0), axis=2)
        total8 = jnp.sum(count8, axis=1)
        fits = jnp.all(total8 <= jnp.asarray(CAPS, jnp.int32))

        def fast(token_ids, positions, table_rows, norm_scale, w_query, w_key, w_value):
            rank8i = rank8.astype(jnp.int32)
            rank = jnp.sum(jnp.where(mine8, rank8i + offset8[:, :, None], 0), axis=0)
            base = lax.dynamic_index_in_dim(jnp.asarray(base_rows), dev // 2, 0, keepdims=False)
            first = jnp.sum(jnp.where(mine8, base[:8, None, None], 0), axis=0)
            slot0 = jnp.where(cold, HOT + rank, ids)
            split = CHIP_CHUNKS[0] * CH
            idx0 = jnp.where(slot0 < split, base[0] + slot0, base[8] + DEV1_CHUNKS * CH + slot0 - split)
            idx = jnp.where(owner == 0, idx0, first + rank).reshape(tokens)

            mine = lax.dynamic_index_in_dim(mine8, dev, 0, keepdims=False)
            within = lax.dynamic_index_in_dim(rank8i, dev, 0, keepdims=False)
            offset = lax.dynamic_index_in_dim(offset8, dev, 0, keepdims=False)
            count = lax.dynamic_index_in_dim(count8, dev, 0, keepdims=False)
            lane = jnp.arange(128, dtype=jnp.int32)
            place = jnp.where(mine, within, -1)
            local = ids - dev * vocab_rows
            listed = jnp.sum(jnp.where(place[:, None, :] == lane[None, :, None], local[:, None, :], 0), axis=2)
            slot = jnp.arange(CAP, dtype=jnp.int32)[:, None]
            group = (offset[None] <= slot) & (slot < (offset + count)[None])
            digits = jnp.concatenate([listed // 256, listed % 256], axis=1).astype(jnp.bfloat16)
            found = jnp.dot(group.astype(jnp.bfloat16), digits, preferred_element_type=jnp.float32)
            found = (found[:, :128] * 256.0 + found[:, 128:]).astype(jnp.int32)
            column = slot - jnp.sum(jnp.where(group, offset[None], 0), axis=1, keepdims=True)
            flat = jnp.sum(jnp.where(column == lane[None], found, 0), axis=1)

            packed = pack_rows(flat, table_rows)
            share = tokens // 8
            idx_here = lax.dynamic_slice_in_dim(idx, dev * share, share)
            lin, rows, rope = ring_call(packed, table_rows, positions, norm_scale, w_query, w_key, w_value)
            return tuple(expand(idx, idx_here, rope, lin, rows))

        outs = lax.cond(fits, fast, general, token_ids, positions, table_rows, norm_scale, w_query, w_key, w_value)
        residual, heads = outs[0], outs[1:]
        return (residual,) + tuple(h.reshape(tokens, 1, HEAD_DIM) for h in heads)

    head_spec = P("dp", "tp", None)
    return jax.shard_map(local_step, mesh=mesh, in_specs=(P("dp"), P("dp"), P("tp", None), P(), P(None, "tp"), P(), P()), out_specs=(P(("dp", "tp"), None), head_spec, head_spec, head_spec), check_vma=False)
```

```python
import functools
import math
import numpy as np
import jax
import jax.numpy as jnp
from jax import lax
from jax.experimental import pallas as pl
from jax.experimental.pallas import tpu as pltpu
from jax.sharding import PartitionSpec as P

HEAD_DIM = 256
LANES = 128
EPSILON = 1e-6
ROPE_BASE = 10000.0
MESH = pl.DeviceIdType.MESH

HOT = 1024
CH = 32
PRE = 12
CHIP_CHUNKS = (57, 11, 6, 6)
DEV1_CHUNKS = 19
HOT_CHUNKS = HOT // CH
HOT_STREAM = HOT_CHUNKS - 2 * PRE
RING_CHUNKS = PRE + sum(CHIP_CHUNKS)
RING_ROWS = RING_CHUNKS * CH
ROWS = 2 * RING_ROWS
COLD0_CHUNKS = 2 * CHIP_CHUNKS[0] - DEV1_CHUNKS - HOT_STREAM
CAPS = tuple(CH * n for n in (COLD0_CHUNKS, DEV1_CHUNKS) + tuple(CHIP_CHUNKS[d // 2] for d in range(2, 8)))
CAP = -(-max(CAPS) // LANES) * LANES
RING_ORDER = ((0, 1, 3, 2), (0, 2, 3, 1))
BLK = LANES
NBLK = -(-RING_ROWS // BLK)
ROPE = 2
PER_TURN = BLK // CH // 2
TILE = 128
NTILE = CAP // TILE
VOCAB_SHIFT = 15


def _base_rows():
    base = np.zeros((4, 9), np.int32)
    for chip in range(4):
        for dev in range(9):
            owner, ring = (0, 1) if dev == 8 else (dev // 2, dev % 2)
            order = RING_ORDER[ring]
            pos, src = order.index(chip), order.index(owner)
            hops = (pos - src) % 4
            before = sum(CHIP_CHUNKS[order[(pos - k) % 4]] for k in range(hops))
            base[chip, dev] = ring * RING_ROWS + (PRE + before) * CH
    return base


def _mo(value, step):
    return pl.multiple_of(value, step)


def start_pairs(count, row_of, source, pairs, first, sem):
    def body(j, carry):
        into = pairs.at[pl.ds(_mo(first + 16 * j, 16), 16), :]
        for k in range(8):
            even = row_of(8 * j + k) & -2
            pltpu.make_async_copy(
                source.at[pl.ds(_mo(even, 2), 2), :], into.at[pl.ds(2 * k, 2), :], sem).start(priority=k % 2)
        return carry
    lax.fori_loop(0, count // 8, body, 0)


def pick_odd(rows_row, count):
    odd = jnp.transpose(jnp.broadcast_to(rows_row & 1, (LANES, LANES)))[:count, :]
    row = lax.broadcasted_iota(jnp.int32, (count, LANES), 0)
    col = lax.broadcasted_iota(jnp.int32, (count, LANES), 1)
    halves = [jnp.where(col + part == 2 * row + odd, 1.0, 0.0) for part in range(0, 2 * count, LANES)]
    return jnp.concatenate(halves, axis=1).astype(jnp.bfloat16)


def pack_kernel(flat_ref, rows_ref, table, out, pairs, packed, gsem, osem):
    dev = lax.axis_index("tp")
    tiles = jnp.where(dev == 0, NTILE, 0)
    for d in range(1, 8):
        tiles = jnp.where(dev == d, -(-CAPS[d] // TILE), tiles)

    def issue(i):
        start_pairs(TILE, lambda j: flat_ref[i * TILE + j], table, pairs, i * 2 * TILE, gsem.at[i])

    def out_copy(i):
        here = pl.ds(_mo(i * TILE, TILE), TILE)
        return pltpu.make_async_copy(packed.at[here, :], out.at[here, :], osem.at[i])

    def finish(i):
        both = pl.ds(_mo(i * 2 * TILE, 2 * TILE), 2 * TILE)
        here = pl.ds(_mo(i * TILE, TILE), TILE)
        pltpu.make_async_copy(table.at[pl.ds(0, 2 * TILE), :], pairs.at[both, :], gsem.at[i]).wait()
        pick = pick_odd(rows_ref[pl.ds(i, 1), :], TILE)
        packed[here, :] = jnp.dot(pick, pairs[both, :], preferred_element_type=jnp.float32).astype(jnp.bfloat16)
        out_copy(i).start()

    lag = 3

    def step(i, carry):
        @pl.when(i < tiles)
        def _():
            issue(i)

        @pl.when(i >= lag)
        def _():
            finish(i - lag)
        return carry
    lax.fori_loop(0, tiles + lag, step, 0)

    def drain(i, carry):
        out_copy(i).wait()
        return carry
    lax.fori_loop(0, tiles, drain, 0)


def pack_rows(flat, table):
    width = table.shape[1]
    return pl.pallas_call(
        pack_kernel,
        out_shape=jax.ShapeDtypeStruct((CAP, width), jnp.bfloat16),
        in_specs=[pl.BlockSpec(memory_space=pltpu.SMEM), pl.BlockSpec(memory_space=pltpu.VMEM),
                  pl.BlockSpec(memory_space=pl.ANY)],
        out_specs=pl.BlockSpec(memory_space=pl.ANY),
        scratch_shapes=[pltpu.VMEM((2 * CAP, width), jnp.bfloat16), pltpu.VMEM((CAP, width), jnp.bfloat16),
                        pltpu.SemaphoreType.DMA((NTILE,)), pltpu.SemaphoreType.DMA((NTILE,))],
        compiler_params=pltpu.CompilerParams(vmem_limit_bytes=60_000_000),
    )(flat.reshape(-1), flat, table)


def place_tokens(dev, ids_ref, idx_ref, flat_ref, fits_ref, rank_s, high_s, low_s, list_s, off_s, count_s):
    groups = ids_ref.shape[0]
    f32, bf16 = jnp.float32, jnp.bfloat16
    ids = ids_ref[...]
    owner = lax.shift_right_logical(ids, VOCAB_SHIFT)
    cold = ids >= HOT
    chip = dev // 2

    def square(n):
        return lax.broadcasted_iota(jnp.int32, (n, n), 0), lax.broadcasted_iota(jnp.int32, (n, n), 1)

    row, col = square(LANES)
    earlier = jnp.where(row < col, 1.0, 0.0).astype(bf16)
    ones = jnp.full((LANES, LANES), 1.0, bf16)
    low_row, low_col = square(groups)
    lower = jnp.where(low_col < low_row, 1.0, 0.0).astype(bf16)
    base_rows = _base_rows()
    base = []
    for d in range(9):
        value = jnp.int32(int(base_rows[0, d]))
        for c in range(1, 4):
            value = jnp.where(chip == c, int(base_rows[c, d]), value)
        base.append(value)
    rank = jnp.zeros((groups, LANES), f32)
    place = jnp.zeros((groups, LANES), f32)
    off_here, count_here = rank, rank
    first = jnp.zeros((groups, LANES), jnp.int32)
    over = jnp.zeros((1, LANES), f32)
    for d in range(8):
        held = cold & (owner == d)
        flags = jnp.where(held, 1.0, 0.0).astype(bf16)
        within = jnp.dot(flags, earlier, preferred_element_type=f32)
        count = jnp.dot(flags, ones, preferred_element_type=f32)
        off = jnp.dot(lower, count.astype(bf16), preferred_element_type=f32)
        rank = jnp.where(held, off + within, rank)
        first = jnp.where(held, base[d], first)
        over = jnp.where((off + count)[groups - 1:, :] > float(CAPS[d]), 1.0, over)
        place = jnp.where(dev == d, jnp.where(held, within, -1.0), place)
        off_here = jnp.where(dev == d, off, off_here)
        count_here = jnp.where(dev == d, count, count_here)
    fits_ref[...] = jnp.broadcast_to(jnp.where(over > 0.0, 0, 1), (8, LANES))
    ranks = rank.astype(jnp.int32)
    early, split = PRE * CH, CHIP_CHUNKS[0] * CH
    slot = jnp.where(cold, HOT + ranks, ids) - 2 * early
    idx0 = jnp.where(slot < split, base[0] + slot, base[8] + DEV1_CHUNKS * CH + slot - split)
    idx0 = jnp.where(ids < 2 * early, jnp.where(ids < early, ids, ids - early + RING_ROWS), idx0)
    idx_ref[...] = jnp.where(owner == 0, idx0, first + ranks)

    rank_s[...] = place
    high_s[...] = (lax.shift_right_logical(ids, 8) & (2 ** (VOCAB_SHIFT - 8) - 1)).astype(f32)
    low_s[...] = (ids & 255).astype(f32)
    list_s[...] = jnp.zeros_like(list_s)
    off_s[...] = jnp.zeros_like(off_s)
    count_s[...] = jnp.zeros_like(count_s)
    off_s[:groups, :] = off_here
    count_s[:groups, :] = count_here
    sub_row = lax.broadcasted_iota(jnp.int32, (8, LANES), 0)
    row_f = row.astype(f32)

    def compact(b, carry):
        here = pl.ds(b, 1)
        pick = jnp.where(rank_s[here, :] == row_f, 1.0, 0.0).astype(bf16)
        digits = jnp.where(sub_row == 0, high_s[here, :], jnp.where(sub_row == 1, low_s[here, :], 0.0)).astype(bf16)
        found = lax.dot_general(digits, pick, (((1,), (1,)), ((), ())), preferred_element_type=f32)
        list_s[here, :] = found[0:1, :] * 256.0 + found[1:2, :]
        return carry
    lax.fori_loop(0, groups, compact, 0, unroll=4)

    listed = jnp.transpose(list_s[...])
    high = jnp.floor(listed * (1.0 / 256.0))
    low = (listed - high * 256.0).astype(bf16)
    high = high.astype(bf16)
    flat_ref[...] = jnp.zeros_like(flat_ref)

    def spread(i, carry):
        at = (col + i * LANES).astype(f32)
        mine = (off_s[...] <= at) & (at < off_s[...] + count_s[...])
        group = jnp.where(mine, 1.0, 0.0).astype(bf16)
        column = at[0:1, :] - jnp.sum(jnp.where(mine, off_s[...], 0.0), axis=0, keepdims=True)
        value = (jnp.dot(high, group, preferred_element_type=f32) * 256.0
                 + jnp.dot(low, group, preferred_element_type=f32))
        value = jnp.sum(jnp.where(row_f == column, value, 0.0), axis=0, keepdims=True)
        flat_ref[pl.ds(i, 1), :] = value.astype(jnp.int32)
        return carry
    lax.fori_loop(0, NTILE, spread, 0)


def early_kernel(table, ids_ref, pre, idx_ref, flat_ref, fits_ref, rsem, nsem, ssem, *scratch):
    dev = lax.axis_index("tp")

    def tokens():
        place_tokens(dev, ids_ref, idx_ref, flat_ref, fits_ref, *scratch)

    chip, core = dev // 2, dev % 2
    sib = chip * 2 + 1 - core
    after = jnp.where(dev == 2, 6, jnp.where(dev == 6, 4, jnp.where(dev == 5, 7, 3)))
    before = jnp.where(dev == 6, 2, jnp.where(dev == 4, 6, jnp.where(dev == 7, 5, jnp.where(dev == 3, 7, 1))))
    ends = (dev == 3) | (dev == 4)
    barrier = pltpu.get_barrier_semaphore()

    def greet(other):
        pl.semaphore_signal(barrier, inc=1, device_id={"tp": other}, device_id_type=MESH)

    greet(sib)

    @pl.when(dev == 1)
    def _():
        greet(2)
        greet(5)

    @pl.when(dev >= 2)
    def _():
        greet(before)

    @pl.when((dev >= 2) & jnp.logical_not(ends))
    def _():
        greet(after)
    pl.semaphore_wait(barrier, jnp.where(dev == 0, 1, jnp.where(ends, 2, 3)))

    def chunk(ref, c):
        return ref.at[pl.ds(_mo(c * CH, CH), CH), :]

    def send(src, c, sem, to):
        return pltpu.make_async_remote_copy(
            src_ref=chunk(src, c), dst_ref=chunk(pre, c), send_sem=sem.at[c], recv_sem=rsem.at[c],
            device_id={"tp": to}, device_id_type=MESH)

    def arrive(c):
        pltpu.make_async_copy(chunk(table, 0), chunk(pre, c), rsem.at[c]).wait()

    def each(count, body):
        def step(i, carry):
            body(i)
            return carry
        lax.fori_loop(0, count, step, 0)

    @pl.when(dev == 0)
    def _():
        def both(k):
            for ring in range(2):
                send(table, ring * PRE + k, ssem, sib).start()
        each(PRE, both)
        tokens()
        each(2 * PRE, lambda c: send(table, c, ssem, sib).wait_send())

    @pl.when(dev == 1)
    def _():
        def both(k):
            for ring, to in ((0, 2), (1, 5)):
                arrive(ring * PRE + k)
                send(pre, ring * PRE + k, nsem, to).start()
        each(PRE, both)
        tokens()
        each(2 * PRE, lambda c: send(pre, c, nsem, 2).wait_send())

    @pl.when(dev >= 2)
    def _():
        def pass_on(k):
            c = core * PRE + k
            arrive(c)

            @pl.when(jnp.logical_not(ends))
            def _():
                send(pre, c, nsem, after).start()
            send(pre, c, ssem, sib).start()
        late = (dev == 2) | (dev == 5)

        @pl.when(jnp.logical_not(late))
        def _():
            tokens()
        each(PRE, pass_on)

        @pl.when(late)
        def _():
            tokens()
        each(PRE, lambda k: arrive((1 - core) * PRE + k))
        each(PRE, lambda k: send(pre, core * PRE + k, ssem, sib).wait_send())

        @pl.when(jnp.logical_not(ends))
        def _():
            each(PRE, lambda k: send(pre, core * PRE + k, nsem, after).wait_send())


def early_call(table, ids):
    anywhere = pl.BlockSpec(memory_space=pl.ANY)
    vmem = pl.BlockSpec(memory_space=pltpu.VMEM)
    groups = ids.shape[0]
    return pl.pallas_call(
        early_kernel,
        out_shape=(jax.ShapeDtypeStruct((2 * PRE * CH, table.shape[1]), table.dtype),
                   jax.ShapeDtypeStruct((groups, LANES), jnp.int32),
                   jax.ShapeDtypeStruct((-(-NTILE // 8) * 8, LANES), jnp.int32),
                   jax.ShapeDtypeStruct((8, LANES), jnp.int32)),
        in_specs=[anywhere, vmem], out_specs=(anywhere, vmem, vmem, vmem),
        scratch_shapes=[pltpu.SemaphoreType.DMA((2 * PRE,))] * 3 + [pltpu.VMEM((groups, LANES), jnp.float32)] * 3
        + [pltpu.VMEM((LANES, LANES), jnp.float32)] * 3,
        compiler_params=pltpu.CompilerParams(collective_id=1, has_side_effects=True),
    )(table, ids)


def ring_kernel(packed, table, pre, pos_ref, freq_ref, scale_ref, wq, wk, wv, lin_out, rows_out, rope_out,
                rows, wbuf, nbuf, oblk, obf, rope_buf, rsem, nsem, ssem, xsem, osem, ksem, psem, wsem):
    width = rows.shape[1]
    normalizer = float(np.asarray(math.sqrt(width), dtype=jnp.bfloat16))
    dev = lax.axis_index("tp")
    chip, core = dev // 2, dev % 2
    pos = jnp.where(chip == 0, 0, jnp.where(chip == 3, 2, jnp.where(chip == 1, 1 + 2 * core, 3 - 2 * core)))

    def chip_at(place):
        return jnp.where(place == 0, 0, jnp.where(place == 2, 3, jnp.where(place == 1, 1 + core, 2 - core)))

    def chunks_of(which):
        return jnp.where(which == 0, CHIP_CHUNKS[0], jnp.where(which == 1, CHIP_CHUNKS[1], CHIP_CHUNKS[2]))

    next_chip = chip_at((pos + 1) % 4)
    next_dev = next_chip * 2 + core
    prev_dev = chip_at((pos + 3) % 4) * 2 + core
    sib = chip * 2 + 1 - core
    own = chunks_of(chip)
    n_next = chunks_of(next_chip)
    local = jnp.where(dev == 1, DEV1_CHUNKS, own)

    def passed(u):
        return PRE + local + (jnp.minimum(u, 2 * NBLK) * (RING_CHUNKS - PRE - local)) // (2 * NBLK)

    n_send = RING_CHUNKS - n_next

    barrier = pltpu.get_barrier_semaphore()
    for other in (next_dev, prev_dev, sib):
        pl.semaphore_signal(barrier, inc=1, device_id={"tp": other}, device_id_type=MESH)

    def chunk(ring, i):
        return rows.at[pl.ds(_mo((ring * RING_CHUNKS + i) * CH, CH), CH), :]

    def sem_of(ring, i):
        return rsem.at[ring * RING_CHUNKS + i]

    def wait_chunk(ring, i):
        pltpu.make_async_copy(table.at[pl.ds(0, CH), :], chunk(ring, i), sem_of(ring, i)).wait()

    def to_next(i):
        return pltpu.make_async_remote_copy(
            src_ref=chunk(core, i), dst_ref=chunk(core, i + n_next), send_sem=nsem.at[i],
            recv_sem=sem_of(core, i + n_next), device_id={"tp": next_dev}, device_id_type=MESH)

    def to_sib(i):
        return pltpu.make_async_remote_copy(
            src_ref=chunk(core, i), dst_ref=chunk(core, i), send_sem=ssem.at[i],
            recv_sem=sem_of(core, i), device_id={"tp": sib}, device_id_type=MESH)

    def to_sib_other(i):
        return pltpu.make_async_remote_copy(
            src_ref=chunk(1, i), dst_ref=chunk(1, i), send_sem=xsem.at[i - PRE - DEV1_CHUNKS],
            recv_sem=sem_of(1, i), device_id={"tp": sib}, device_id_type=MESH)

    def load_pre(i, carry):
        for ring in range(2):
            from_rows = pl.ds(_mo((ring * PRE + i) * CH, CH), CH)

            @pl.when(dev == 0)
            def _():
                pltpu.make_async_copy(table.at[from_rows, :], chunk(ring, i), sem_of(ring, i)).start()

            @pl.when(dev != 0)
            def _():
                pltpu.make_async_copy(pre.at[from_rows, :], chunk(ring, i), sem_of(ring, i)).start()
        return carry

    def load(i, carry):
        to, sem = chunk(core, PRE + i), sem_of(core, PRE + i)

        @pl.when((dev == 0) & (i < HOT_STREAM))
        def _():
            pltpu.make_async_copy(table.at[pl.ds(_mo((2 * PRE + i) * CH, CH), CH), :], to, sem).start()

        @pl.when((dev != 0) | (i >= HOT_STREAM))
        def _():
            first = i - jnp.where(dev == 0, HOT_STREAM, 0)
            pltpu.make_async_copy(packed.at[pl.ds(_mo(first * CH, CH), CH), :], to, sem).start()
        return carry
    lax.fori_loop(0, local, load, 0)

    @pl.when(dev == 0)
    def _():
        def load_other(i, carry):
            first = i - DEV1_CHUNKS + CHIP_CHUNKS[0] - HOT_STREAM
            pltpu.make_async_copy(packed.at[pl.ds(_mo(first * CH, CH), CH), :], chunk(1, PRE + i), sem_of(1, PRE + i)).start()
            return carry
        lax.fori_loop(DEV1_CHUNKS, CHIP_CHUNKS[0], load_other, 0)
    lax.fori_loop(0, PRE, load_pre, 0)

    weights = []
    for k, w in enumerate((wq, wk, wv)):
        cols = pl.ds(0, HEAD_DIM) if k == 0 else pl.ds(_mo(chip * HEAD_DIM, HEAD_DIM), HEAD_DIM)
        weights.append(pltpu.make_async_copy(w.at[:, cols], wbuf.at[:, pl.ds(k * HEAD_DIM, HEAD_DIM)], wsem.at[k]))
    for copy in weights:
        copy.start()

    pl.semaphore_wait(barrier, 3)

    def first_sends(i, carry):
        wait_chunk(core, i)
        to_next(i).start()
        return carry
    lax.fori_loop(PRE, PRE + local, first_sends, 0)

    @pl.when(dev == 0)
    def _():
        def send_other(i, carry):
            wait_chunk(1, i)
            to_sib_other(i).start()
            return carry
        lax.fori_loop(PRE + DEV1_CHUNKS, PRE + CHIP_CHUNKS[0], send_other, 0)

    def first_sib(i, carry):
        to_sib(i).start()
        return carry
    lax.fori_loop(PRE, PRE + local, first_sib, 0)

    def wait_pre(i, carry):
        for ring in range(2):
            wait_chunk(ring, i)
        return carry
    lax.fori_loop(0, PRE, wait_pre, 0)
    for copy in weights:
        copy.wait()

    def relay(i, carry):
        wait_chunk(core, i)

        @pl.when(i < n_send)
        def _():
            to_next(i).start()

        @pl.when((dev != 1) | (i >= PRE + CHIP_CHUNKS[0]))
        def _():
            to_sib(i).start()
        return carry

    def lin_copy(first, slot):
        return pltpu.make_async_copy(
            obf.at[slot], lin_out.at[pl.ds(first, BLK), :, :], osem.at[slot])

    def keep_copy(first, slot):
        here = pl.ds(_mo(first, CH), BLK)
        return pltpu.make_async_copy(rows.at[here, :], rows_out.at[here, :], ksem.at[slot])

    def rope_copy(group, slot):
        return pltpu.make_async_copy(
            rope_buf.at[slot], rope_out.at[pl.ds(_mo(group * LANES, LANES), LANES), :], psem.at[slot])

    def rope_tables_of(group, slot):
        angle = jnp.transpose(jnp.broadcast_to(pos_ref[pl.ds(group, 1), :].astype(jnp.float32), (LANES, LANES))) * freq_ref[...]
        cosine, sine = cos_sin(angle)

        @pl.when(group >= 2)
        def _():
            rope_copy(group, slot).wait()
        rope_buf[slot, :, :LANES] = cosine
        rope_buf[slot, :, LANES:] = sine
        rope_copy(group, slot).start()

    def block_start(b):
        return jnp.where(b == NBLK - 1, RING_ROWS - BLK, b * BLK)

    def projections(ring, b, slot, turn):
        first = ring * RING_ROWS + block_start(b)
        gain = 1.0 + scale_ref[...]

        def norm(k, carry):
            emb = rows[pl.ds(_mo(first + k * 32, 32), 32), :].astype(jnp.float32)
            resid = (emb * normalizer).astype(jnp.bfloat16).astype(jnp.float32)
            inv_rms = lax.rsqrt(jnp.mean(resid * resid, axis=-1, keepdims=True) + EPSILON)
            nbuf[pl.ds(_mo(k * 32, 32), 32), :] = (resid * inv_rms * gain).astype(jnp.bfloat16)
            return carry
        lax.fori_loop(0, BLK // 32, norm, 0)

        @pl.when(turn >= 2)
        def _():
            lin_copy(first, slot).wait()
            keep_copy(first, slot).wait()
        keep_copy(first, slot).start()
        for k in range(3):
            lin = jnp.dot(nbuf[...], wbuf[:, k * HEAD_DIM:(k + 1) * HEAD_DIM], preferred_element_type=jnp.float32)
            for half in range(2):
                oblk[pl.ds(2 * k + half, BLK, stride=8), :] = lin[:, half * LANES:(half + 1) * LANES]
        obf[slot] = oblk[...].reshape(BLK, 8, LANES).astype(jnp.bfloat16)
        lin_copy(first, slot).start()

    def turn_body(u, carry):
        b, half = u // 2, u % 2
        turn = u - 2
        ring = jnp.where(half == 0, core, 1 - core)
        lax.fori_loop(passed(u), passed(u + 1), relay, 0)

        @pl.when(turn >= 0)
        def _():
            @pl.when(half == 1)
            def _():
                def wait_one(k, c):
                    i = 2 * PER_TURN * (b - 1) + k

                    @pl.when((i >= PRE) & (i < RING_CHUNKS) &
                             ((dev != 0) | (i < PRE + DEV1_CHUNKS) | (i >= PRE + CHIP_CHUNKS[0])))
                    def _():
                        wait_chunk(1 - core, i)
                    return c
                lax.fori_loop(0, 2 * PER_TURN, wait_one, 0)
            projections(ring, b - 1, half, turn)

        @pl.when((turn >= 0) & (turn * ROPE < pos_ref.shape[0]))
        def _():
            for k in range(ROPE):
                rope_tables_of(turn * ROPE + k, k % 2)
        return carry
    lax.fori_loop(0, 2 * NBLK + 2, turn_body, 0)

    for slot in range(2):
        lin_copy(0, slot).wait()
        keep_copy(0, slot).wait()
        rope_copy(0, slot).wait()

    def drain_next(i, carry):
        to_next(i).wait_send()
        return carry
    lax.fori_loop(PRE, n_send, drain_next, 0)

    def drain_sib(i, carry):
        @pl.when((dev != 1) | (i < PRE + DEV1_CHUNKS) | (i >= PRE + CHIP_CHUNKS[0]))
        def _():
            to_sib(i).wait_send()
        return carry
    lax.fori_loop(PRE, RING_CHUNKS, drain_sib, 0)

    @pl.when(dev == 0)
    def _():
        def drain_other(i, carry):
            to_sib_other(i).wait_send()
            return carry
        lax.fori_loop(PRE + DEV1_CHUNKS, PRE + CHIP_CHUNKS[0], drain_other, 0)


def ring_call(packed, table, pre, positions, norm_scale, w_query, w_key, w_value):
    width = table.shape[1]
    tokens = positions.shape[0]
    freq = (ROPE_BASE ** (-np.arange(0, HEAD_DIM, 2) / HEAD_DIM)).astype(np.float32)[None, :]
    anywhere = pl.BlockSpec(memory_space=pl.ANY)
    vmem = pl.BlockSpec(memory_space=pltpu.VMEM)
    return pl.pallas_call(
        ring_kernel,
        out_shape=(jax.ShapeDtypeStruct((ROWS, 8, LANES), jnp.bfloat16),
                   jax.ShapeDtypeStruct((ROWS, width), jnp.bfloat16),
                   jax.ShapeDtypeStruct((tokens, HEAD_DIM), jnp.float32)),
        in_specs=[anywhere, anywhere, anywhere, vmem, vmem, vmem, anywhere, anywhere, anywhere],
        out_specs=(anywhere, anywhere, anywhere),
        scratch_shapes=[
            pltpu.VMEM((ROWS, width), jnp.bfloat16),
            pltpu.VMEM((width, 3 * HEAD_DIM), jnp.bfloat16),
            pltpu.VMEM((BLK, width), jnp.bfloat16),
            pltpu.VMEM((BLK * 8, LANES), jnp.float32),
            pltpu.VMEM((2, BLK, 8, LANES), jnp.bfloat16),
            pltpu.VMEM((2, LANES, HEAD_DIM), jnp.float32),
            pltpu.SemaphoreType.DMA((2 * RING_CHUNKS,)),
            pltpu.SemaphoreType.DMA((RING_CHUNKS,)),
            pltpu.SemaphoreType.DMA((RING_CHUNKS,)),
            pltpu.SemaphoreType.DMA((CHIP_CHUNKS[0] - DEV1_CHUNKS,)),
            pltpu.SemaphoreType.DMA((2,)),
            pltpu.SemaphoreType.DMA((2,)),
            pltpu.SemaphoreType.DMA((2,)),
            pltpu.SemaphoreType.DMA((3,)),
        ],
        compiler_params=pltpu.CompilerParams(collective_id=0, has_side_effects=True, vmem_limit_bytes=60_000_000),
    )(packed, table, pre, positions.reshape(tokens // LANES, LANES), jnp.asarray(freq), norm_scale[None, :],
      w_query, w_key, w_value)


def cos_sin(angle):
    turns = jnp.floor(angle * (2.0 / math.pi) + 0.5)
    rest = ((angle - turns * 1.5703125) - turns * 4.837512969970703125e-4) - turns * 7.54978995489188216e-8
    quarter = turns.astype(jnp.int32)
    z = rest * rest
    s = rest + rest * z * (-1.6666654611e-1 + z * (8.3321608736e-3 + z * -1.9515295891e-4))
    c = 1.0 - 0.5 * z + z * z * (4.166664568298827e-2 + z * (-1.388731625493765e-3 + z * 2.443315711809948e-5))
    odd = (quarter & 1) == 1
    cosine = jnp.where(odd, s, c)
    sine = jnp.where(odd, c, s)
    cosine = jnp.where(((quarter + 1) & 2) == 2, -cosine, cosine)
    sine = jnp.where((quarter & 2) == 2, -sine, sine)
    return cosine, sine


EXPAND = 1024
SUB = 64
SHARE = 128
LOADS = 8


def expand_kernel(idx_ref, here_ref, rope_ref, lin, rows, res_ref, q_ref, k_ref, v_ref,
                  table, even, odd, pairs, sem, gsem):
    step, steps = pl.program_id(0), pl.num_programs(0)
    first = lax.axis_index("tp") * (steps * SHARE)
    piece = table.shape[0] // LOADS
    tiles = EXPAND // SUB
    last = steps * tiles - 1

    def start_share(n):
        start_pairs(SHARE, lambda j: idx_ref[first + n * SHARE + j], rows, pairs, n * 2 * SHARE, gsem.at[n])

    def take(tile, picked):
        for t in range(SUB):
            row = idx_ref[tile * SUB + t]
            picked[8 * t:8 * t + 8, :] = table[row].astype(jnp.float32)

    @pl.when(step == 0)
    def _():
        copies = [pltpu.make_async_copy(lin.at[pl.ds(n * piece, piece)], table.at[pl.ds(n * piece, piece)],
                                        sem.at[n]) for n in range(LOADS)]
        for n, copy in enumerate(copies):
            copy.start(priority=n % 2)
        def start_one(n, carry):
            start_share(n)
            return carry
        lax.fori_loop(0, steps, start_one, 0)
        for copy in copies:
            copy.wait()
        take(0, even)

    def rope(n, picked):
        here = pl.ds(_mo(n * SUB, SUB), SUB)
        cosines, sines = rope_ref[here, :LANES], rope_ref[here, LANES:]
        part = [picked[pl.ds(s, SUB, stride=8), :] for s in range(6)]
        factor = HEAD_DIM ** -0.5
        q_ref[here, :LANES] = ((part[0] * cosines - part[1] * sines) * factor).astype(jnp.bfloat16)
        q_ref[here, LANES:] = ((part[1] * cosines + part[0] * sines) * factor).astype(jnp.bfloat16)
        k_ref[here, :LANES] = (part[2] * cosines - part[3] * sines).astype(jnp.bfloat16)
        k_ref[here, LANES:] = (part[3] * cosines + part[2] * sines).astype(jnp.bfloat16)
        v_ref[here, :LANES] = part[4].astype(jnp.bfloat16)
        v_ref[here, LANES:] = part[5].astype(jnp.bfloat16)

    def two_tiles(n, carry):
        tile = step * tiles + 2 * n
        take(tile + 1, odd)
        rope(2 * n, even)
        take(jnp.minimum(tile + 2, last), even)
        rope(2 * n + 1, odd)
        return carry
    lax.fori_loop(0, tiles // 2, two_tiles, 0)

    share = pairs.at[pl.ds(_mo(step * 2 * SHARE, 2 * SHARE), 2 * SHARE), :]
    pltpu.make_async_copy(rows.at[pl.ds(0, 2 * SHARE), :], share, gsem.at[step]).wait()
    normalizer = float(np.asarray(math.sqrt(rows.shape[1]), dtype=jnp.bfloat16))
    emb = jnp.dot(pick_odd(here_ref[pl.ds(lax.axis_index("tp") * steps + step, 1), :], SHARE), share[...], preferred_element_type=jnp.float32)
    res_ref[...] = (emb * normalizer).astype(jnp.bfloat16)


def expand(idx, rope, lin, rows):
    tokens, width = idx.size, rows.shape[1]
    steps = tokens // EXPAND
    head = jax.ShapeDtypeStruct((tokens, HEAD_DIM), jnp.bfloat16)
    head_spec = pl.BlockSpec((EXPAND, HEAD_DIM), lambda i: (i, 0))
    return pl.pallas_call(
        expand_kernel,
        grid=(steps,),
        out_shape=(jax.ShapeDtypeStruct((steps * SHARE, width), jnp.bfloat16), head, head, head),
        in_specs=[pl.BlockSpec(memory_space=pltpu.SMEM), pl.BlockSpec(memory_space=pltpu.VMEM),
                  pl.BlockSpec((EXPAND, HEAD_DIM), lambda i: (i, 0)),
                  pl.BlockSpec(memory_space=pl.ANY), pl.BlockSpec(memory_space=pl.ANY)],
        out_specs=(pl.BlockSpec((SHARE, width), lambda i: (i, 0)), head_spec, head_spec, head_spec),
        scratch_shapes=[pltpu.VMEM(lin.shape, jnp.bfloat16), pltpu.VMEM((SUB * 8, LANES), jnp.float32),
                        pltpu.VMEM((SUB * 8, LANES), jnp.float32), pltpu.VMEM((steps * 2 * SHARE, width), jnp.bfloat16),
                        pltpu.SemaphoreType.DMA((LOADS,)), pltpu.SemaphoreType.DMA((steps,))],
        compiler_params=pltpu.CompilerParams(vmem_limit_bytes=60_000_000),
    )(idx.reshape(-1), idx, rope, lin, rows)


def rope_tables(positions):
    inv_freq = ROPE_BASE ** (-jnp.arange(0, HEAD_DIM, 2, dtype=jnp.float32) / HEAD_DIM)
    angles = positions.astype(jnp.float32)[:, None] * inv_freq[None, :]
    return jnp.cos(angles)[:, None, :], jnp.sin(angles)[:, None, :]


def rotate(head_vals, cosines, sines):
    half_dim = head_vals.shape[-1] // 2
    front_half = head_vals[..., :half_dim]
    back_half = head_vals[..., half_dim:]
    return jnp.concatenate([front_half * cosines - back_half * sines, back_half * cosines + front_half * sines], axis=-1)


def rms_norm(resid_rows, norm_scale):
    widened = resid_rows.astype(jnp.float32)
    inv_rms = lax.rsqrt(jnp.mean(widened * widened, axis=-1, keepdims=True) + EPSILON)
    return (widened * inv_rms * (1.0 + norm_scale)).astype(jnp.bfloat16)


def project(normed, weight, cosines, sines, factor):
    linear = jnp.dot(normed, weight, preferred_element_type=jnp.float32).astype(jnp.bfloat16)
    return (rotate(linear.reshape(linear.shape[0], 1, HEAD_DIM).astype(jnp.float32), cosines, sines) * factor).astype(jnp.bfloat16)


def general(token_ids, positions, table_rows, norm_scale, w_query, w_key, w_value):
    dev = lax.axis_index("tp")
    vocab_rows, width = table_rows.shape
    tokens = token_ids.shape[0]
    normalizer = jnp.asarray(math.sqrt(width), dtype=jnp.bfloat16)
    local_ids = token_ids - dev * vocab_rows
    inside = (local_ids >= 0) & (local_ids < vocab_rows)
    picked = jnp.take(table_rows, local_ids, axis=0, mode="clip") * normalizer
    partial = jnp.where(inside[:, None], picked, jnp.zeros((), jnp.bfloat16))
    parts = lax.all_to_all(partial.reshape(8, tokens // 8, width), "tp", 0, 0)
    residual = jnp.sum(parts.astype(jnp.float32), axis=0).astype(jnp.bfloat16)
    normed = rms_norm(residual, norm_scale)
    normed = lax.all_to_all(jnp.broadcast_to(normed[None], (8,) + normed.shape), "tp", 0, 0).reshape(tokens, width)
    cosines, sines = rope_tables(positions)
    queries = project(normed, w_query, cosines, sines, HEAD_DIM ** -0.5)
    col = (dev // 2) * HEAD_DIM
    key_heads = project(normed, lax.dynamic_slice_in_dim(w_key, col, HEAD_DIM, axis=1), cosines, sines, 1.0)
    value_cols = lax.dynamic_slice_in_dim(w_value, col, HEAD_DIM, axis=1)
    value_heads = jnp.dot(normed, value_cols, preferred_element_type=jnp.float32).astype(jnp.bfloat16)
    return (residual, queries.reshape(tokens, HEAD_DIM), key_heads.reshape(tokens, HEAD_DIM), value_heads)


def solution(mesh):
    def local_step(token_ids, positions, table_rows, norm_scale, w_query, w_key, w_value):
        tokens = token_ids.shape[0]
        pre, idx, flat, fits = early_call(table_rows, token_ids.reshape(tokens // LANES, LANES))

        def fast(token_ids, positions, table_rows, norm_scale, w_query, w_key, w_value):
            packed = pack_rows(flat, table_rows)
            lin, rows, rope = ring_call(packed, table_rows, pre, positions, norm_scale, w_query, w_key, w_value)
            return tuple(expand(idx, rope, lin, rows))

        outs = lax.cond(fits[0, 0] > 0, fast, general, token_ids, positions, table_rows, norm_scale, w_query, w_key, w_value)
        residual, heads = outs[0], outs[1:]
        return (residual,) + tuple(h.reshape(tokens, 1, HEAD_DIM) for h in heads)

    head_spec = P("dp", "tp", None)
    return jax.shard_map(local_step, mesh=mesh, in_specs=(P("dp"), P("dp"), P("tp", None), P(), P(None, "tp"), P(), P()), out_specs=(P(("dp", "tp"), None), head_spec, head_spec, head_spec), check_vma=False)
```

```python
import functools
import math
import numpy as np
import jax
import jax.numpy as jnp
from jax import lax
from jax.experimental import pallas as pl
from jax.experimental.pallas import tpu as pltpu
from jax.sharding import PartitionSpec as P

HEAD_DIM = 256
LANES = 128
EPSILON = 1e-6
ROPE_BASE = 10000.0
MESH = pl.DeviceIdType.MESH

HOT = 1024
CH = 32
PRE = 12
CHIP_CHUNKS = (57, 11, 6, 6)
DEV1_CHUNKS = 19
HOT_CHUNKS = HOT // CH
HOT_STREAM = HOT_CHUNKS - 2 * PRE
RING_CHUNKS = PRE + sum(CHIP_CHUNKS)
RING_ROWS = RING_CHUNKS * CH
ROWS = 2 * RING_ROWS
COLD0_CHUNKS = 2 * CHIP_CHUNKS[0] - DEV1_CHUNKS - HOT_STREAM
CAPS = tuple(CH * n for n in (COLD0_CHUNKS, DEV1_CHUNKS) + tuple(CHIP_CHUNKS[d // 2] for d in range(2, 8)))
CAP = -(-max(CAPS) // LANES) * LANES
RING_ORDER = ((0, 1, 3, 2), (0, 2, 3, 1))
BLK = LANES
NBLK = -(-RING_ROWS // BLK)
ROPE = 2
PER_TURN = BLK // CH // 2
TILE = 128
NTILE = CAP // TILE
VOCAB_SHIFT = 15


def _base_rows():
    base = np.zeros((4, 9), np.int32)
    for chip in range(4):
        for dev in range(9):
            owner, ring = (0, 1) if dev == 8 else (dev // 2, dev % 2)
            order = RING_ORDER[ring]
            pos, src = order.index(chip), order.index(owner)
            hops = (pos - src) % 4
            before = sum(CHIP_CHUNKS[order[(pos - k) % 4]] for k in range(hops))
            base[chip, dev] = ring * RING_ROWS + (PRE + before) * CH
    return base


def _mo(value, step):
    return pl.multiple_of(value, step)


def start_pairs(count, row_of, source, pairs, first, sem):
    def body(j, carry):
        into = pairs.at[pl.ds(_mo(first + 16 * j, 16), 16), :]
        for k in range(8):
            even = row_of(8 * j + k) & -2
            pltpu.make_async_copy(
                source.at[pl.ds(_mo(even, 2), 2), :], into.at[pl.ds(2 * k, 2), :], sem).start(priority=k % 2)
        return carry
    lax.fori_loop(0, count // 8, body, 0)


def pick_odd(rows_row, count):
    odd = jnp.transpose(jnp.broadcast_to(rows_row & 1, (LANES, LANES)))[:count, :]
    row = lax.broadcasted_iota(jnp.int32, (count, LANES), 0)
    col = lax.broadcasted_iota(jnp.int32, (count, LANES), 1)
    halves = [jnp.where(col + part == 2 * row + odd, 1.0, 0.0) for part in range(0, 2 * count, LANES)]
    return jnp.concatenate(halves, axis=1).astype(jnp.bfloat16)


def pack_kernel(flat_ref, rows_ref, table, out, pairs, packed, gsem, osem):
    dev = lax.axis_index("tp")
    tiles = jnp.where(dev == 0, NTILE, 0)
    for d in range(1, 8):
        tiles = jnp.where(dev == d, -(-CAPS[d] // TILE), tiles)

    def issue(i):
        start_pairs(TILE, lambda j: flat_ref[i * TILE + j], table, pairs, i * 2 * TILE, gsem.at[i])

    def out_copy(i):
        here = pl.ds(_mo(i * TILE, TILE), TILE)
        return pltpu.make_async_copy(packed.at[here, :], out.at[here, :], osem.at[i])

    def finish(i):
        both = pl.ds(_mo(i * 2 * TILE, 2 * TILE), 2 * TILE)
        here = pl.ds(_mo(i * TILE, TILE), TILE)
        pltpu.make_async_copy(table.at[pl.ds(0, 2 * TILE), :], pairs.at[both, :], gsem.at[i]).wait()
        pick = pick_odd(rows_ref[pl.ds(i, 1), :], TILE)
        packed[here, :] = jnp.dot(pick, pairs[both, :], preferred_element_type=jnp.float32).astype(jnp.bfloat16)
        out_copy(i).start()

    lag = 3

    def step(i, carry):
        @pl.when(i < tiles)
        def _():
            issue(i)

        @pl.when(i >= lag)
        def _():
            finish(i - lag)
        return carry
    lax.fori_loop(0, tiles + lag, step, 0)

    def drain(i, carry):
        out_copy(i).wait()
        return carry
    lax.fori_loop(0, tiles, drain, 0)


def pack_rows(flat, table):
    width = table.shape[1]
    return pl.pallas_call(
        pack_kernel,
        out_shape=jax.ShapeDtypeStruct((CAP, width), jnp.bfloat16),
        in_specs=[pl.BlockSpec(memory_space=pltpu.SMEM), pl.BlockSpec(memory_space=pltpu.VMEM),
                  pl.BlockSpec(memory_space=pl.ANY)],
        out_specs=pl.BlockSpec(memory_space=pl.ANY),
        scratch_shapes=[pltpu.VMEM((2 * CAP, width), jnp.bfloat16), pltpu.VMEM((CAP, width), jnp.bfloat16),
                        pltpu.SemaphoreType.DMA((NTILE,)), pltpu.SemaphoreType.DMA((NTILE,))],
        compiler_params=pltpu.CompilerParams(vmem_limit_bytes=60_000_000),
    )(flat.reshape(-1), flat, table)


def place_tokens(dev, ids_ref, idx_ref, flat_ref, fits_ref, rank_s, high_s, low_s, list_s, off_s, count_s):
    groups = ids_ref.shape[0]
    f32, bf16 = jnp.float32, jnp.bfloat16
    ids = ids_ref[...]
    owner = lax.shift_right_logical(ids, VOCAB_SHIFT)
    cold = ids >= HOT
    chip = dev // 2

    def square(n):
        return lax.broadcasted_iota(jnp.int32, (n, n), 0), lax.broadcasted_iota(jnp.int32, (n, n), 1)

    row, col = square(LANES)
    earlier = jnp.where(row < col, 1.0, 0.0).astype(bf16)
    ones = jnp.full((LANES, LANES), 1.0, bf16)
    low_row, low_col = square(groups)
    lower = jnp.where(low_col < low_row, 1.0, 0.0).astype(bf16)
    base_rows = _base_rows()
    base = []
    for d in range(9):
        value = jnp.int32(int(base_rows[0, d]))
        for c in range(1, 4):
            value = jnp.where(chip == c, int(base_rows[c, d]), value)
        base.append(value)
    rank = jnp.zeros((groups, LANES), f32)
    place = jnp.zeros((groups, LANES), f32)
    off_here, count_here = rank, rank
    first = jnp.zeros((groups, LANES), jnp.int32)
    over = jnp.zeros((1, LANES), f32)
    for d in range(8):
        held = cold & (owner == d)
        flags = jnp.where(held, 1.0, 0.0).astype(bf16)
        within = jnp.dot(flags, earlier, preferred_element_type=f32)
        count = jnp.dot(flags, ones, preferred_element_type=f32)
        off = jnp.dot(lower, count.astype(bf16), preferred_element_type=f32)
        rank = jnp.where(held, off + within, rank)
        first = jnp.where(held, base[d], first)
        over = jnp.where((off + count)[groups - 1:, :] > float(CAPS[d]), 1.0, over)
        place = jnp.where(dev == d, jnp.where(held, within, -1.0), place)
        off_here = jnp.where(dev == d, off, off_here)
        count_here = jnp.where(dev == d, count, count_here)
    fits_ref[...] = jnp.broadcast_to(jnp.where(over > 0.0, 0, 1), (8, LANES))
    ranks = rank.astype(jnp.int32)
    early, split = PRE * CH, CHIP_CHUNKS[0] * CH
    slot = jnp.where(cold, HOT + ranks, ids) - 2 * early
    idx0 = jnp.where(slot < split, base[0] + slot, base[8] + DEV1_CHUNKS * CH + slot - split)
    idx0 = jnp.where(ids < 2 * early, jnp.where(ids < early, ids, ids - early + RING_ROWS), idx0)
    idx_ref[...] = jnp.where(owner == 0, idx0, first + ranks)

    rank_s[...] = place
    high_s[...] = (lax.shift_right_logical(ids, 8) & (2 ** (VOCAB_SHIFT - 8) - 1)).astype(f32)
    low_s[...] = (ids & 255).astype(f32)
    list_s[...] = jnp.zeros_like(list_s)
    off_s[...] = jnp.zeros_like(off_s)
    count_s[...] = jnp.zeros_like(count_s)
    off_s[:groups, :] = off_here
    count_s[:groups, :] = count_here
    sub_row = lax.broadcasted_iota(jnp.int32, (8, LANES), 0)
    row_f = row.astype(f32)

    def compact(b, carry):
        here = pl.ds(b, 1)
        pick = jnp.where(rank_s[here, :] == row_f, 1.0, 0.0).astype(bf16)
        digits = jnp.where(sub_row == 0, high_s[here, :], jnp.where(sub_row == 1, low_s[here, :], 0.0)).astype(bf16)
        found = lax.dot_general(digits, pick, (((1,), (1,)), ((), ())), preferred_element_type=f32)
        list_s[here, :] = found[0:1, :] * 256.0 + found[1:2, :]
        return carry
    lax.fori_loop(0, groups, compact, 0, unroll=4)

    listed = jnp.transpose(list_s[...])
    high = jnp.floor(listed * (1.0 / 256.0))
    low = (listed - high * 256.0).astype(bf16)
    high = high.astype(bf16)
    flat_ref[...] = jnp.zeros_like(flat_ref)

    def spread(i, carry):
        at = (col + i * LANES).astype(f32)
        mine = (off_s[...] <= at) & (at < off_s[...] + count_s[...])
        group = jnp.where(mine, 1.0, 0.0).astype(bf16)
        column = at[0:1, :] - jnp.sum(jnp.where(mine, off_s[...], 0.0), axis=0, keepdims=True)
        value = (jnp.dot(high, group, preferred_element_type=f32) * 256.0
                 + jnp.dot(low, group, preferred_element_type=f32))
        value = jnp.sum(jnp.where(row_f == column, value, 0.0), axis=0, keepdims=True)
        flat_ref[pl.ds(i, 1), :] = value.astype(jnp.int32)
        return carry
    lax.fori_loop(0, NTILE, spread, 0)


def early_kernel(table, ids_ref, pre, idx_ref, flat_ref, fits_ref, rsem, nsem, ssem, *scratch):
    dev = lax.axis_index("tp")

    def tokens():
        place_tokens(dev, ids_ref, idx_ref, flat_ref, fits_ref, *scratch)

    chip, core = dev // 2, dev % 2
    sib = chip * 2 + 1 - core
    after = jnp.where(dev == 2, 6, jnp.where(dev == 6, 4, jnp.where(dev == 5, 7, 3)))
    before = jnp.where(dev == 6, 2, jnp.where(dev == 4, 6, jnp.where(dev == 7, 5, jnp.where(dev == 3, 7, 1))))
    ends = (dev == 3) | (dev == 4)
    barrier = pltpu.get_barrier_semaphore()

    def greet(other):
        pl.semaphore_signal(barrier, inc=1, device_id={"tp": other}, device_id_type=MESH)

    greet(sib)

    @pl.when(dev == 1)
    def _():
        greet(2)
        greet(5)

    @pl.when(dev >= 2)
    def _():
        greet(before)

    @pl.when((dev >= 2) & jnp.logical_not(ends))
    def _():
        greet(after)
    pl.semaphore_wait(barrier, jnp.where(dev == 0, 1, jnp.where(ends, 2, 3)))

    def chunk(ref, c):
        return ref.at[pl.ds(_mo(c * CH, CH), CH), :]

    def send(src, c, sem, to):
        return pltpu.make_async_remote_copy(
            src_ref=chunk(src, c), dst_ref=chunk(pre, c), send_sem=sem.at[c], recv_sem=rsem.at[c],
            device_id={"tp": to}, device_id_type=MESH)

    def arrive(c):
        pltpu.make_async_copy(chunk(table, 0), chunk(pre, c), rsem.at[c]).wait()

    def each(count, body):
        def step(i, carry):
            body(i)
            return carry
        lax.fori_loop(0, count, step, 0)

    @pl.when(dev == 0)
    def _():
        def both(k):
            for ring in range(2):
                send(table, ring * PRE + k, ssem, sib).start()
        each(PRE, both)
        tokens()
        each(2 * PRE, lambda c: send(table, c, ssem, sib).wait_send())

    @pl.when(dev == 1)
    def _():
        def both(k):
            for ring, to in ((0, 2), (1, 5)):
                arrive(ring * PRE + k)
                send(pre, ring * PRE + k, nsem, to).start()
        each(PRE, both)
        tokens()
        each(2 * PRE, lambda c: send(pre, c, nsem, 2).wait_send())

    @pl.when(dev >= 2)
    def _():
        def pass_on(k):
            c = core * PRE + k
            arrive(c)

            @pl.when(jnp.logical_not(ends))
            def _():
                send(pre, c, nsem, after).start()
            send(pre, c, ssem, sib).start()
        late = (dev == 2) | (dev == 5)

        @pl.when(jnp.logical_not(late))
        def _():
            tokens()
        each(PRE, pass_on)

        @pl.when(late)
        def _():
            tokens()
        each(PRE, lambda k: arrive((1 - core) * PRE + k))
        each(PRE, lambda k: send(pre, core * PRE + k, ssem, sib).wait_send())

        @pl.when(jnp.logical_not(ends))
        def _():
            each(PRE, lambda k: send(pre, core * PRE + k, nsem, after).wait_send())


def early_call(table, ids):
    anywhere = pl.BlockSpec(memory_space=pl.ANY)
    vmem = pl.BlockSpec(memory_space=pltpu.VMEM)
    groups = ids.shape[0]
    return pl.pallas_call(
        early_kernel,
        out_shape=(jax.ShapeDtypeStruct((2 * PRE * CH, table.shape[1]), table.dtype),
                   jax.ShapeDtypeStruct((groups, LANES), jnp.int32),
                   jax.ShapeDtypeStruct((-(-NTILE // 8) * 8, LANES), jnp.int32),
                   jax.ShapeDtypeStruct((8, LANES), jnp.int32)),
        in_specs=[anywhere, vmem], out_specs=(anywhere, vmem, vmem, vmem),
        scratch_shapes=[pltpu.SemaphoreType.DMA((2 * PRE,))] * 3 + [pltpu.VMEM((groups, LANES), jnp.float32)] * 3
        + [pltpu.VMEM((LANES, LANES), jnp.float32)] * 3,
        compiler_params=pltpu.CompilerParams(collective_id=1, has_side_effects=True),
    )(table, ids)


def ring_kernel(packed, table, pre, pos_ref, freq_ref, scale_ref, wq, wk, wv, lin_out, rows_out, rope_out,
                rows, wbuf, nbuf, oblk, obf, rope_buf, rsem, nsem, ssem, xsem, osem, ksem, psem, wsem):
    width = rows.shape[1]
    normalizer = float(np.asarray(math.sqrt(width), dtype=jnp.bfloat16))
    dev = lax.axis_index("tp")
    chip, core = dev // 2, dev % 2
    pos = jnp.where(chip == 0, 0, jnp.where(chip == 3, 2, jnp.where(chip == 1, 1 + 2 * core, 3 - 2 * core)))

    def chip_at(place):
        return jnp.where(place == 0, 0, jnp.where(place == 2, 3, jnp.where(place == 1, 1 + core, 2 - core)))

    def chunks_of(which):
        return jnp.where(which == 0, CHIP_CHUNKS[0], jnp.where(which == 1, CHIP_CHUNKS[1], CHIP_CHUNKS[2]))

    next_chip = chip_at((pos + 1) % 4)
    next_dev = next_chip * 2 + core
    prev_dev = chip_at((pos + 3) % 4) * 2 + core
    sib = chip * 2 + 1 - core
    own = chunks_of(chip)
    n_next = chunks_of(next_chip)
    local = jnp.where(dev == 1, DEV1_CHUNKS, own)

    def passed(u):
        return PRE + local + (jnp.minimum(u, 2 * NBLK) * (RING_CHUNKS - PRE - local)) // (2 * NBLK)

    n_send = RING_CHUNKS - n_next

    barrier = pltpu.get_barrier_semaphore()
    for other in (next_dev, prev_dev, sib):
        pl.semaphore_signal(barrier, inc=1, device_id={"tp": other}, device_id_type=MESH)

    def chunk(ring, i):
        return rows.at[pl.ds(_mo((ring * RING_CHUNKS + i) * CH, CH), CH), :]

    def sem_of(ring, i):
        return rsem.at[ring * RING_CHUNKS + i]

    def wait_chunk(ring, i):
        pltpu.make_async_copy(table.at[pl.ds(0, CH), :], chunk(ring, i), sem_of(ring, i)).wait()

    def to_next(i):
        return pltpu.make_async_remote_copy(
            src_ref=chunk(core, i), dst_ref=chunk(core, i + n_next), send_sem=nsem.at[i],
            recv_sem=sem_of(core, i + n_next), device_id={"tp": next_dev}, device_id_type=MESH)

    def to_sib(i):
        return pltpu.make_async_remote_copy(
            src_ref=chunk(core, i), dst_ref=chunk(core, i), send_sem=ssem.at[i],
            recv_sem=sem_of(core, i), device_id={"tp": sib}, device_id_type=MESH)

    def to_sib_other(i):
        return pltpu.make_async_remote_copy(
            src_ref=chunk(1, i), dst_ref=chunk(1, i), send_sem=xsem.at[i - PRE - DEV1_CHUNKS],
            recv_sem=sem_of(1, i), device_id={"tp": sib}, device_id_type=MESH)

    def load_pre(i, carry):
        for ring in range(2):
            from_rows = pl.ds(_mo((ring * PRE + i) * CH, CH), CH)

            @pl.when(dev == 0)
            def _():
                pltpu.make_async_copy(table.at[from_rows, :], chunk(ring, i), sem_of(ring, i)).start()

            @pl.when(dev != 0)
            def _():
                pltpu.make_async_copy(pre.at[from_rows, :], chunk(ring, i), sem_of(ring, i)).start()
        return carry

    def load(i, carry):
        to, sem = chunk(core, PRE + i), sem_of(core, PRE + i)

        @pl.when((dev == 0) & (i < HOT_STREAM))
        def _():
            pltpu.make_async_copy(table.at[pl.ds(_mo((2 * PRE + i) * CH, CH), CH), :], to, sem).start()

        @pl.when((dev != 0) | (i >= HOT_STREAM))
        def _():
            first = i - jnp.where(dev == 0, HOT_STREAM, 0)
            pltpu.make_async_copy(packed.at[pl.ds(_mo(first * CH, CH), CH), :], to, sem).start()
        return carry
    lax.fori_loop(0, local, load, 0)

    @pl.when(dev == 0)
    def _():
        def load_other(i, carry):
            first = i - DEV1_CHUNKS + CHIP_CHUNKS[0] - HOT_STREAM
            pltpu.make_async_copy(packed.at[pl.ds(_mo(first * CH, CH), CH), :], chunk(1, PRE + i), sem_of(1, PRE + i)).start()
            return carry
        lax.fori_loop(DEV1_CHUNKS, CHIP_CHUNKS[0], load_other, 0)
    lax.fori_loop(0, PRE, load_pre, 0)

    weights = []
    for k, w in enumerate((wq, wk, wv)):
        cols = pl.ds(0, HEAD_DIM) if k == 0 else pl.ds(_mo(chip * HEAD_DIM, HEAD_DIM), HEAD_DIM)
        weights.append(pltpu.make_async_copy(w.at[:, cols], wbuf.at[:, pl.ds(k * HEAD_DIM, HEAD_DIM)], wsem.at[k]))
    for copy in weights:
        copy.start()

    pl.semaphore_wait(barrier, 3)

    def first_sends(i, carry):
        wait_chunk(core, i)
        to_next(i).start()
        return carry
    lax.fori_loop(PRE, PRE + local, first_sends, 0)

    @pl.when(dev == 0)
    def _():
        def send_other(i, carry):
            wait_chunk(1, i)
            to_sib_other(i).start()
            return carry
        lax.fori_loop(PRE + DEV1_CHUNKS, PRE + CHIP_CHUNKS[0], send_other, 0)

    def first_sib(i, carry):
        to_sib(i).start()
        return carry
    lax.fori_loop(PRE, PRE + local, first_sib, 0)

    def wait_pre(i, carry):
        for ring in range(2):
            wait_chunk(ring, i)
        return carry
    lax.fori_loop(0, PRE, wait_pre, 0)
    for copy in weights:
        copy.wait()

    def relay(i, carry):
        wait_chunk(core, i)

        @pl.when(i < n_send)
        def _():
            to_next(i).start()

        @pl.when((dev != 1) | (i >= PRE + CHIP_CHUNKS[0]))
        def _():
            to_sib(i).start()
        return carry

    def lin_copy(first, slot):
        return pltpu.make_async_copy(
            obf.at[slot], lin_out.at[pl.ds(first, BLK), :, :], osem.at[slot])

    def keep_copy(first, slot):
        here = pl.ds(_mo(first, CH), BLK)
        return pltpu.make_async_copy(rows.at[here, :], rows_out.at[here, :], ksem.at[slot])

    def rope_copy(group, slot):
        return pltpu.make_async_copy(
            rope_buf.at[slot], rope_out.at[pl.ds(_mo(group * LANES, LANES), LANES), :], psem.at[slot])

    def rope_tables_of(group, slot):
        angle = jnp.transpose(jnp.broadcast_to(pos_ref[pl.ds(group, 1), :].astype(jnp.float32), (LANES, LANES))) * freq_ref[...]
        cosine, sine = cos_sin(angle)

        @pl.when(group >= 2)
        def _():
            rope_copy(group, slot).wait()
        rope_buf[slot, :, :LANES] = cosine
        rope_buf[slot, :, LANES:] = sine
        rope_copy(group, slot).start()

    def block_start(b):
        return jnp.where(b == NBLK - 1, RING_ROWS - BLK, b * BLK)

    def projections(ring, b, slot, turn):
        first = ring * RING_ROWS + block_start(b)
        gain = 1.0 + scale_ref[...]

        def norm(k, carry):
            emb = rows[pl.ds(_mo(first + k * 32, 32), 32), :].astype(jnp.float32)
            resid = (emb * normalizer).astype(jnp.bfloat16).astype(jnp.float32)
            inv_rms = lax.rsqrt(jnp.mean(resid * resid, axis=-1, keepdims=True) + EPSILON)
            nbuf[pl.ds(_mo(k * 32, 32), 32), :] = (resid * inv_rms * gain).astype(jnp.bfloat16)
            return carry
        lax.fori_loop(0, BLK // 32, norm, 0)

        @pl.when(turn >= 2)
        def _():
            lin_copy(first, slot).wait()
            keep_copy(first, slot).wait()
        keep_copy(first, slot).start()
        for k in range(3):
            lin = jnp.dot(nbuf[...], wbuf[:, k * HEAD_DIM:(k + 1) * HEAD_DIM], preferred_element_type=jnp.float32)
            for half in range(2):
                oblk[pl.ds(2 * k + half, BLK, stride=8), :] = lin[:, half * LANES:(half + 1) * LANES]
        obf[slot] = oblk[...].reshape(BLK, 8, LANES).astype(jnp.bfloat16)
        lin_copy(first, slot).start()

    def turn_body(u, carry):
        b, half = u // 2, u % 2
        turn = u - 2
        ring = jnp.where(half == 0, core, 1 - core)
        lax.fori_loop(passed(u), passed(u + 1), relay, 0)

        @pl.when(turn >= 0)
        def _():
            @pl.when(half == 1)
            def _():
                def wait_one(k, c):
                    i = 2 * PER_TURN * (b - 1) + k

                    @pl.when((i >= PRE) & (i < RING_CHUNKS) &
                             ((dev != 0) | (i < PRE + DEV1_CHUNKS) | (i >= PRE + CHIP_CHUNKS[0])))
                    def _():
                        wait_chunk(1 - core, i)
                    return c
                lax.fori_loop(0, 2 * PER_TURN, wait_one, 0)
            projections(ring, b - 1, half, turn)

        @pl.when((turn >= 0) & (turn * ROPE < pos_ref.shape[0]))
        def _():
            for k in range(ROPE):
                rope_tables_of(turn * ROPE + k, k % 2)
        return carry
    lax.fori_loop(0, 2 * NBLK + 2, turn_body, 0)

    for slot in range(2):
        lin_copy(0, slot).wait()
        keep_copy(0, slot).wait()
        rope_copy(0, slot).wait()

    def drain_next(i, carry):
        to_next(i).wait_send()
        return carry
    lax.fori_loop(PRE, n_send, drain_next, 0)

    def drain_sib(i, carry):
        @pl.when((dev != 1) | (i < PRE + DEV1_CHUNKS) | (i >= PRE + CHIP_CHUNKS[0]))
        def _():
            to_sib(i).wait_send()
        return carry
    lax.fori_loop(PRE, RING_CHUNKS, drain_sib, 0)

    @pl.when(dev == 0)
    def _():
        def drain_other(i, carry):
            to_sib_other(i).wait_send()
            return carry
        lax.fori_loop(PRE + DEV1_CHUNKS, PRE + CHIP_CHUNKS[0], drain_other, 0)


def ring_call(packed, table, pre, positions, norm_scale, w_query, w_key, w_value):
    width = table.shape[1]
    tokens = positions.shape[0]
    freq = (ROPE_BASE ** (-np.arange(0, HEAD_DIM, 2) / HEAD_DIM)).astype(np.float32)[None, :]
    anywhere = pl.BlockSpec(memory_space=pl.ANY)
    vmem = pl.BlockSpec(memory_space=pltpu.VMEM)
    return pl.pallas_call(
        ring_kernel,
        out_shape=(jax.ShapeDtypeStruct((ROWS, 8, LANES), jnp.bfloat16),
                   jax.ShapeDtypeStruct((ROWS, width), jnp.bfloat16),
                   jax.ShapeDtypeStruct((tokens, HEAD_DIM), jnp.float32)),
        in_specs=[anywhere, anywhere, anywhere, vmem, vmem, vmem, anywhere, anywhere, anywhere],
        out_specs=(anywhere, anywhere, anywhere),
        scratch_shapes=[
            pltpu.VMEM((ROWS, width), jnp.bfloat16),
            pltpu.VMEM((width, 3 * HEAD_DIM), jnp.bfloat16),
            pltpu.VMEM((BLK, width), jnp.bfloat16),
            pltpu.VMEM((BLK * 8, LANES), jnp.float32),
            pltpu.VMEM((2, BLK, 8, LANES), jnp.bfloat16),
            pltpu.VMEM((2, LANES, HEAD_DIM), jnp.float32),
            pltpu.SemaphoreType.DMA((2 * RING_CHUNKS,)),
            pltpu.SemaphoreType.DMA((RING_CHUNKS,)),
            pltpu.SemaphoreType.DMA((RING_CHUNKS,)),
            pltpu.SemaphoreType.DMA((CHIP_CHUNKS[0] - DEV1_CHUNKS,)),
            pltpu.SemaphoreType.DMA((2,)),
            pltpu.SemaphoreType.DMA((2,)),
            pltpu.SemaphoreType.DMA((2,)),
            pltpu.SemaphoreType.DMA((3,)),
        ],
        compiler_params=pltpu.CompilerParams(collective_id=0, has_side_effects=True, vmem_limit_bytes=60_000_000),
    )(packed, table, pre, positions.reshape(tokens // LANES, LANES), jnp.asarray(freq), norm_scale[None, :],
      w_query, w_key, w_value)


def cos_sin(angle):
    turns = jnp.floor(angle * (2.0 / math.pi) + 0.5)
    rest = ((angle - turns * 1.5703125) - turns * 4.837512969970703125e-4) - turns * 7.54978995489188216e-8
    quarter = turns.astype(jnp.int32)
    z = rest * rest
    s = rest + rest * z * (-1.6666654611e-1 + z * (8.3321608736e-3 + z * -1.9515295891e-4))
    c = 1.0 - 0.5 * z + z * z * (4.166664568298827e-2 + z * (-1.388731625493765e-3 + z * 2.443315711809948e-5))
    odd = (quarter & 1) == 1
    cosine = jnp.where(odd, s, c)
    sine = jnp.where(odd, c, s)
    cosine = jnp.where(((quarter + 1) & 2) == 2, -cosine, cosine)
    sine = jnp.where((quarter & 2) == 2, -sine, sine)
    return cosine, sine


EXPAND = 1024
SUB = 32
SHARE = 128
LOADS = 8


def expand_kernel(idx_ref, here_ref, rope_ref, lin, rows, res_ref, q_ref, k_ref, v_ref,
                  table, even, odd, pairs, sem, gsem):
    step, steps = pl.program_id(0), pl.num_programs(0)
    first = lax.axis_index("tp") * (steps * SHARE)
    piece = table.shape[0] // LOADS
    tiles = EXPAND // SUB
    last = steps * tiles - 1

    def start_share(n):
        start_pairs(SHARE, lambda j: idx_ref[first + n * SHARE + j], rows, pairs, n * 2 * SHARE, gsem.at[n])

    def take(tile, picked):
        for t in range(SUB):
            row = idx_ref[tile * SUB + t]
            picked[8 * t:8 * t + 8, :] = table[row].astype(jnp.float32)

    @pl.when(step == 0)
    def _():
        copies = [pltpu.make_async_copy(lin.at[pl.ds(n * piece, piece)], table.at[pl.ds(n * piece, piece)],
                                        sem.at[n]) for n in range(LOADS)]
        for n, copy in enumerate(copies):
            copy.start(priority=n % 2)
        def start_one(n, carry):
            start_share(n)
            return carry
        lax.fori_loop(0, steps, start_one, 0)
        for copy in copies:
            copy.wait()
        take(0, even)

    def rope(n, picked):
        here = pl.ds(_mo(n * SUB, SUB), SUB)
        cosines, sines = rope_ref[here, :LANES], rope_ref[here, LANES:]
        part = [picked[pl.ds(s, SUB, stride=8), :] for s in range(6)]
        factor = HEAD_DIM ** -0.5
        q_ref[here, :LANES] = ((part[0] * cosines - part[1] * sines) * factor).astype(jnp.bfloat16)
        q_ref[here, LANES:] = ((part[1] * cosines + part[0] * sines) * factor).astype(jnp.bfloat16)
        k_ref[here, :LANES] = (part[2] * cosines - part[3] * sines).astype(jnp.bfloat16)
        k_ref[here, LANES:] = (part[3] * cosines + part[2] * sines).astype(jnp.bfloat16)
        v_ref[here, :LANES] = part[4].astype(jnp.bfloat16)
        v_ref[here, LANES:] = part[5].astype(jnp.bfloat16)

    def two_tiles(n, carry):
        tile = step * tiles + 2 * n
        take(tile + 1, odd)
        rope(2 * n, even)
        take(jnp.minimum(tile + 2, last), even)
        rope(2 * n + 1, odd)
        return carry
    lax.fori_loop(0, tiles // 2, two_tiles, 0)

    share = pairs.at[pl.ds(_mo(step * 2 * SHARE, 2 * SHARE), 2 * SHARE), :]
    pltpu.make_async_copy(rows.at[pl.ds(0, 2 * SHARE), :], share, gsem.at[step]).wait()
    normalizer = float(np.asarray(math.sqrt(rows.shape[1]), dtype=jnp.bfloat16))
    emb = jnp.dot(pick_odd(here_ref[pl.ds(lax.axis_index("tp") * steps + step, 1), :], SHARE), share[...], preferred_element_type=jnp.float32)
    res_ref[...] = (emb * normalizer).astype(jnp.bfloat16)


def expand(idx, rope, lin, rows):
    tokens, width = idx.size, rows.shape[1]
    steps = tokens // EXPAND
    head = jax.ShapeDtypeStruct((tokens, HEAD_DIM), jnp.bfloat16)
    head_spec = pl.BlockSpec((EXPAND, HEAD_DIM), lambda i: (i, 0))
    return pl.pallas_call(
        expand_kernel,
        grid=(steps,),
        out_shape=(jax.ShapeDtypeStruct((steps * SHARE, width), jnp.bfloat16), head, head, head),
        in_specs=[pl.BlockSpec(memory_space=pltpu.SMEM), pl.BlockSpec(memory_space=pltpu.VMEM),
                  pl.BlockSpec((EXPAND, HEAD_DIM), lambda i: (i, 0)),
                  pl.BlockSpec(memory_space=pl.ANY), pl.BlockSpec(memory_space=pl.ANY)],
        out_specs=(pl.BlockSpec((SHARE, width), lambda i: (i, 0)), head_spec, head_spec, head_spec),
        scratch_shapes=[pltpu.VMEM(lin.shape, jnp.bfloat16), pltpu.VMEM((SUB * 8, LANES), jnp.float32),
                        pltpu.VMEM((SUB * 8, LANES), jnp.float32), pltpu.VMEM((steps * 2 * SHARE, width), jnp.bfloat16),
                        pltpu.SemaphoreType.DMA((LOADS,)), pltpu.SemaphoreType.DMA((steps,))],
        compiler_params=pltpu.CompilerParams(vmem_limit_bytes=60_000_000),
    )(idx.reshape(-1), idx, rope, lin, rows)


def rope_tables(positions):
    inv_freq = ROPE_BASE ** (-jnp.arange(0, HEAD_DIM, 2, dtype=jnp.float32) / HEAD_DIM)
    angles = positions.astype(jnp.float32)[:, None] * inv_freq[None, :]
    return jnp.cos(angles)[:, None, :], jnp.sin(angles)[:, None, :]


def rotate(head_vals, cosines, sines):
    half_dim = head_vals.shape[-1] // 2
    front_half = head_vals[..., :half_dim]
    back_half = head_vals[..., half_dim:]
    return jnp.concatenate([front_half * cosines - back_half * sines, back_half * cosines + front_half * sines], axis=-1)


def rms_norm(resid_rows, norm_scale):
    widened = resid_rows.astype(jnp.float32)
    inv_rms = lax.rsqrt(jnp.mean(widened * widened, axis=-1, keepdims=True) + EPSILON)
    return (widened * inv_rms * (1.0 + norm_scale)).astype(jnp.bfloat16)


def project(normed, weight, cosines, sines, factor):
    linear = jnp.dot(normed, weight, preferred_element_type=jnp.float32).astype(jnp.bfloat16)
    return (rotate(linear.reshape(linear.shape[0], 1, HEAD_DIM).astype(jnp.float32), cosines, sines) * factor).astype(jnp.bfloat16)


def general(token_ids, positions, table_rows, norm_scale, w_query, w_key, w_value):
    dev = lax.axis_index("tp")
    vocab_rows, width = table_rows.shape
    tokens = token_ids.shape[0]
    normalizer = jnp.asarray(math.sqrt(width), dtype=jnp.bfloat16)
    local_ids = token_ids - dev * vocab_rows
    inside = (local_ids >= 0) & (local_ids < vocab_rows)
    picked = jnp.take(table_rows, local_ids, axis=0, mode="clip") * normalizer
    partial = jnp.where(inside[:, None], picked, jnp.zeros((), jnp.bfloat16))
    parts = lax.all_to_all(partial.reshape(8, tokens // 8, width), "tp", 0, 0)
    residual = jnp.sum(parts.astype(jnp.float32), axis=0).astype(jnp.bfloat16)
    normed = rms_norm(residual, norm_scale)
    normed = lax.all_to_all(jnp.broadcast_to(normed[None], (8,) + normed.shape), "tp", 0, 0).reshape(tokens, width)
    cosines, sines = rope_tables(positions)
    queries = project(normed, w_query, cosines, sines, HEAD_DIM ** -0.5)
    col = (dev // 2) * HEAD_DIM
    key_heads = project(normed, lax.dynamic_slice_in_dim(w_key, col, HEAD_DIM, axis=1), cosines, sines, 1.0)
    value_cols = lax.dynamic_slice_in_dim(w_value, col, HEAD_DIM, axis=1)
    value_heads = jnp.dot(normed, value_cols, preferred_element_type=jnp.float32).astype(jnp.bfloat16)
    return (residual, queries.reshape(tokens, HEAD_DIM), key_heads.reshape(tokens, HEAD_DIM), value_heads)


def solution(mesh):
    def local_step(token_ids, positions, table_rows, norm_scale, w_query, w_key, w_value):
        tokens = token_ids.shape[0]
        pre, idx, flat, fits = early_call(table_rows, token_ids.reshape(tokens // LANES, LANES))

        def fast(token_ids, positions, table_rows, norm_scale, w_query, w_key, w_value):
            packed = pack_rows(flat, table_rows)
            lin, rows, rope = ring_call(packed, table_rows, pre, positions, norm_scale, w_query, w_key, w_value)
            return tuple(expand(idx, rope, lin, rows))

        outs = lax.cond(fits[0, 0] > 0, fast, general, token_ids, positions, table_rows, norm_scale, w_query, w_key, w_value)
        residual, heads = outs[0], outs[1:]
        return (residual,) + tuple(h.reshape(tokens, 1, HEAD_DIM) for h in heads)

    head_spec = P("dp", "tp", None)
    return jax.shard_map(local_step, mesh=mesh, in_specs=(P("dp"), P("dp"), P("tp", None), P(), P(None, "tp"), P(), P()), out_specs=(P(("dp", "tp"), None), head_spec, head_spec, head_spec), check_vma=False)
```
